32 devices in a mesh: groups: 2 (over y), gz: 8 (over z, x), ea: 2 (over core).
Axes of the slice: x: 2, y: 2, z: 4, core: 2. Of those that a mesh axis runs over, the one named last changes fastest.
Arguments:
- eigvec: bfloat16 [96, 3, 2, 16, 512], P('ea', None, None, ('groups', 'gz')), parts along dimension 3, may hold values from -3 to 3
- links: float32 [3, 3, 3, 2, 16, 512], P(None, None, None, None, ('groups', 'gz')), parts along dimension 4, may hold values from -1.8 to 1.8
- momentum: int32 [6], P('groups'), parts along dimension 0, may hold values from -2 to 2
- weights: int32 [6], P('groups'), parts along dimension 0, may hold values from 1 to 3
- spins: int32 [6, 2], P('groups'), parts along dimension 0, may hold values from 0 to 3
- peram: float32 [8, 4, 2, 96, 96], P('groups'), parts along dimension 0, may hold values from -0.4375 to 0.4375
Outputs:
- baryon_block: float32 [4, 96, 9216], P('groups', 'ea', 'gz'), parts along dimension 0
The draws below stay inside these ranges and needn't reach their ends.
There are 2 independent parts, one for each index of `groups`. The reference program is written for one: setup_inputs(seed, part) draws one part's arguments, and reference() takes and returns one part's arrays. A program takes and returns all parts, laid end to end along the dimension named above; each array names one. Nothing has to cross between parts.
All inputs are finite; a program needn't handle non-finite values.
Results may differ from the reference program's by a relative error of at most 0.0045.
Values may be sent and summed in bfloat16 or wider, within the bound.
A program may use at most 64 MiB of HBM per device.

```python
import math
import jax
import jax.numpy as jnp
from jax import lax

NVEC = 96
LX = 32
LY = 16
NSPIN = 4
PLANE = 512
NZ = 8
VOLUME = 4096


def set_ends(values, stream_key, smallest, largest):
    place = [jax.random.randint(jax.random.fold_in(stream_key, axis), (), 0, length) for axis, length in enumerate(values.shape)]
    longest = values.shape.index(max(values.shape))
    neighbour = place[:longest] + [(place[longest] + 1) % values.shape[longest]] + place[longest + 1:]
    return values.at[tuple(place)].set(smallest).at[tuple(neighbour)].set(largest)


def levels(rng, dims, cuts, least, largest):
    loudness, own = 1.0, jax.random.fold_in(rng, 6)
    for axis_at, blocks in cuts:
        draws = jnp.exp(jax.random.uniform(jax.random.fold_in(own, axis_at), (blocks,), jnp.float32, least / len(cuts), largest / len(cuts)))
        loudness = loudness * jnp.repeat(draws, dims[axis_at] // blocks).reshape([-1 if axis == axis_at else 1 for axis in range(len(dims))])
    return loudness


def scatter_about(rng, shape, scale, limit, split=(), held_as=jnp.bfloat16):
    array = jax.random.normal(rng, shape, jnp.float32) * scale
    if len(split) > 0:
        array = levels(rng, shape, split, -0.22, 0.18) * array
    return jnp.clip(array, min=-limit, max=limit).astype(held_as)


def setup_inputs(seed: int = 0, part: int = 0) -> dict:
    arg_keys = jax.random.split(jax.random.key(seed), 7)
    part_keys = jax.random.split(jax.random.fold_in(arg_keys[6], part), 7)
    eigvec = scatter_about(part_keys[0], (NVEC, 3, 2, NZ, PLANE), 0.5, 3.0, ((0, 2), (3, 8)))
    links = scatter_about(part_keys[1], (3, 3, 3, 2, NZ, PLANE), 0.3, 1.8, ((4, 8),), jnp.float32)
    momentum = jax.random.randint(part_keys[2], (3,), -2, 3).astype(jnp.int32)
    weights = jax.random.randint(part_keys[3], (3,), 1, 4).astype(jnp.int32)
    spins = set_ends(jax.random.randint(part_keys[4], (3, 2), 0, 4), jax.random.fold_in(part_keys[4], 1), 0, 3).astype(jnp.int32)
    peram = scatter_about(part_keys[5], (NSPIN, NSPIN, 2, NVEC, NVEC), (2 * NVEC) ** -0.5, 0.4375, (), jnp.float32)
    return dict(eigvec=eigvec, links=links, momentum=momentum, weights=weights, spins=spins, peram=peram)


def link_apply(link, lattice_field):
    result_real = 0.0
    result_imaginary = 0.0
    for column_slot in range(3):
        gauge_link_real = link[None, :, column_slot, 0]
        gauge_link_imaginary = link[None, :, column_slot, 1]
        vector_real = lattice_field[:, None, column_slot, 0]
        vector_imaginary = lattice_field[:, None, column_slot, 1]
        result_real = result_real + gauge_link_real * vector_real - gauge_link_imaginary * vector_imaginary
        result_imaginary = result_imaginary + gauge_link_real * vector_imaginary + gauge_link_imaginary * vector_real
    return jnp.stack([result_real, result_imaginary], 2)

def adjoint_apply(link, lattice_field):
    result_real = 0.0
    result_imaginary = 0.0
    for column_slot in range(3):
        gauge_link_real = link[None, column_slot, :, 0]
        gauge_link_imaginary = link[None, column_slot, :, 1]
        vector_real = lattice_field[:, None, column_slot, 0]
        vector_imaginary = lattice_field[:, None, column_slot, 1]
        result_real = result_real + gauge_link_real * vector_real + gauge_link_imaginary * vector_imaginary
        result_imaginary = result_imaginary + gauge_link_real * vector_imaginary - gauge_link_imaginary * vector_real
    return jnp.stack([result_real, result_imaginary], 2)

def cross_parts(left_vec, right_vec):
    reals = []
    imags = []
    for first, second in ((1, 2), (2, 0), (0, 1)):
        ar = left_vec[:, :, first, 0]
        ai = left_vec[:, :, first, 1]
        br = left_vec[:, :, second, 0]
        bi = left_vec[:, :, second, 1]
        cr = right_vec[:, :, first, 0]
        ci = right_vec[:, :, first, 1]
        dr = right_vec[:, :, second, 0]
        di = right_vec[:, :, second, 1]
        reals.append(ar * dr - ai * di - (br * cr - bi * ci))
        imags.append(ar * di + ai * dr - (br * ci + bi * cr))
    return jnp.stack([jnp.stack(reals), jnp.stack(imags)])

def mode_product(lattice_field, block, form):
    high = lax.Precision.HIGHEST
    real_part = jnp.einsum(form, lattice_field[0], block[0], precision=high) - jnp.einsum(form, lattice_field[1], block[1], precision=high)
    imag_part = jnp.einsum(form, lattice_field[0], block[1], precision=high) + jnp.einsum(form, lattice_field[1], block[0], precision=high)
    return jnp.stack([real_part, imag_part])

def reference(eigvec, links, momentum, weights, spins, peram):
    vecf = eigvec.astype(jnp.float32)
    shape_full = vecf.shape[:4] + (LY, LX)
    grid = vecf.reshape(shape_full)
    linkgrid = links.reshape(links.shape[:5] + (LY, LX))
    axes_of = (5, 4, 3)
    disp = jnp.zeros(shape_full, jnp.float32)
    for direction in range(3):
        link = linkgrid[direction]
        ahead = jnp.roll(grid, -1, axes_of[direction])
        back = adjoint_apply(link, grid).astype(jnp.bfloat16)
        behind = jnp.roll(back, 1, axes_of[direction])
        behind = lax.optimization_barrier(behind).astype(jnp.float32)
        factor = weights[direction].astype(jnp.float32)
        disp = disp + factor * (link_apply(link, ahead) - behind)
    disp = disp.reshape(vecf.shape)
    sites = jnp.arange(PLANE, dtype=jnp.int32)
    xcoord = sites % LX
    ycoord = sites // LX
    zcoord = jnp.arange(NZ, dtype=jnp.int32)
    two_pi = 2.0 * math.pi
    inplane = (momentum[0] * xcoord).astype(jnp.float32) / LX + (momentum[1] * ycoord).astype(jnp.float32) / LY
    angle = two_pi * inplane[None, :] + two_pi * (momentum[2] * zcoord).astype(jnp.float32)[:, None] / NZ
    cosine = jnp.cos(angle)
    sine = jnp.sin(angle)
    phased_re = cosine * disp[:, :, 0] + sine * disp[:, :, 1]
    phased_im = cosine * disp[:, :, 1] - sine * disp[:, :, 0]
    phased = jnp.stack([phased_re, phased_im], 2).astype(jnp.bfloat16).astype(jnp.float32)
    high = lax.Precision.HIGHEST

    def plane_step(total, planes):
        vplane, dplane = planes
        wmat = cross_parts(vplane[:, None], vplane[None]).astype(jnp.bfloat16)
        wmat = lax.optimization_barrier(wmat).astype(jnp.float32)
        lre = dplane[:, :, 0]
        lim = dplane[:, :, 1]
        ere = jnp.einsum('aks,kbcs->abc', lre, wmat[0], precision=high) - jnp.einsum('aks,kbcs->abc', lim, wmat[1], precision=high)
        eim = jnp.einsum('aks,kbcs->abc', lre, wmat[1], precision=high) + jnp.einsum('aks,kbcs->abc', lim, wmat[0], precision=high)
        return (total + jnp.stack([ere, eim]), None)
    start = jnp.zeros((2, NVEC, NVEC, NVEC), jnp.float32)
    elemental, unused = lax.scan(plane_step, start, (jnp.moveaxis(vecf, 3, 0), jnp.moveaxis(phased, 3, 0)))
    elemental = elemental * (1.0 / math.sqrt(VOLUME))
    blocks = [peram[spins[q, 0], spins[q, 1]] for q in range(3)]
    result = mode_product(elemental, blocks[2], 'abc,cf->abf')
    result = mode_product(result, blocks[1], 'abc,be->aec')
    result = mode_product(result, blocks[0], 'abc,ad->dbc')
    return result.reshape(2, NVEC, NVEC * NVEC)
```

```python
import functools
import math

import jax
import jax.numpy as jnp
from jax import lax
from jax.experimental import pallas as pl
from jax.experimental.pallas import tpu as pltpu
from jax.sharding import PartitionSpec as P

LX = 32
LY = 16
F32 = jnp.float32
BF16 = jnp.bfloat16
NT = (((1,), (0,)), ((), ()))


def from_behind(array, axis, by):
    count = lax.axis_size(axis)
    return lax.ppermute(array, axis, [(i, (i + by) % count) for i in range(count)])


def plain_link(link, lattice_field):
    result_real = 0.0
    result_imaginary = 0.0
    for column_slot in range(3):
        gauge_link_real = link[None, :, column_slot, 0]
        gauge_link_imaginary = link[None, :, column_slot, 1]
        vector_real = lattice_field[:, None, column_slot, 0]
        vector_imaginary = lattice_field[:, None, column_slot, 1]
        result_real = (
            result_real + gauge_link_real * vector_real - gauge_link_imaginary * vector_imaginary
        )
        result_imaginary = (
            result_imaginary
            + gauge_link_real * vector_imaginary
            + gauge_link_imaginary * vector_real
        )
    return jnp.stack([result_real, result_imaginary], 2)


def adjoint_apply(link, lattice_field):
    result_real = 0.0
    result_imaginary = 0.0
    for column_slot in range(3):
        gauge_link_real = link[None, column_slot, :, 0]
        gauge_link_imaginary = link[None, column_slot, :, 1]
        vector_real = lattice_field[:, None, column_slot, 0]
        vector_imaginary = lattice_field[:, None, column_slot, 1]
        result_real = (
            result_real + gauge_link_real * vector_real + gauge_link_imaginary * vector_imaginary
        )
        result_imaginary = (
            result_imaginary
            + gauge_link_real * vector_imaginary
            - gauge_link_imaginary * vector_real
        )
    return jnp.stack([result_real, result_imaginary], 2)


def cross_parts(left_vec, right_vec):
    reals = []
    imags = []
    for first, second in ((1, 2), (2, 0), (0, 1)):
        ar = left_vec[:, :, first, 0]
        ai = left_vec[:, :, first, 1]
        br = left_vec[:, :, second, 0]
        bi = left_vec[:, :, second, 1]
        cr = right_vec[:, :, first, 0]
        ci = right_vec[:, :, first, 1]
        dr = right_vec[:, :, second, 0]
        di = right_vec[:, :, second, 1]
        reals.append(ar * dr - ai * di - (br * cr - bi * ci))
        imags.append(ar * di + ai * dr - (br * ci + bi * cr))
    return jnp.stack([jnp.stack(reals), jnp.stack(imags)])


def mode_product(lattice_field, block, form):
    high = lax.Precision.HIGHEST
    real_part = jnp.einsum(form, lattice_field[0], block[0], precision=high) - jnp.einsum(
        form, lattice_field[1], block[1], precision=high
    )
    imag_part = jnp.einsum(form, lattice_field[0], block[1], precision=high) + jnp.einsum(
        form, lattice_field[1], block[0], precision=high
    )
    return jnp.stack([real_part, imag_part])


def roll_plane(lattice_field, direction, amount):
    grid = lattice_field.reshape(lattice_field.shape[:-1] + (LY, LX))
    axis_here = grid.ndim - 1 if direction == 0 else grid.ndim - 2
    return jnp.roll(grid, amount, axis_here).reshape(lattice_field.shape)


def elemental_part(phased, vectors):
    count = vectors.shape[0]
    size_a = phased.shape[0]
    nsites = vectors.shape[3]
    real_part = phased[:, :, 0]
    imag_part = phased[:, :, 1]
    upper_rows = jnp.stack([real_part, -imag_part], 1)
    lower_rows = jnp.stack([imag_part, real_part], 1)
    left = jnp.stack([upper_rows, lower_rows], 0).reshape(2 * size_a, 2, 3, nsites)
    width = min(8, count)
    others = vectors.astype(jnp.float32)[None]

    def one_block(rows):
        wmat = cross_parts(rows.astype(jnp.float32)[:, None], others).astype(jnp.bfloat16)
        return jnp.einsum("xrks,rkbcs->xbc", left, wmat, preferred_element_type=jnp.float32)

    result = lax.map(one_block, vectors.reshape(count // width, width, 3, 2, nsites))
    return result.transpose(1, 0, 2, 3).reshape(2, size_a, count * count)


def plain_shards(eigvec, links, momentum, weights, spins, peram):
    local_vecs = eigvec.shape[0]
    planes = eigvec.shape[3]
    plane = eigvec.shape[4]
    depth = planes * lax.axis_size("gz")
    vecf = eigvec.astype(jnp.float32)
    disp = jnp.zeros(vecf.shape, jnp.float32)
    for direction in range(3):
        link = links[direction]
        back = adjoint_apply(link, vecf).astype(jnp.bfloat16)
        if direction == 2:
            upper = from_behind(eigvec, "gz", -1)
            ahead = jnp.concatenate([eigvec[:, :, :, 1:], upper], axis=3).astype(jnp.float32)
            lower = from_behind(back, "gz", 1)
            behind = jnp.concatenate([lower, back[:, :, :, :-1]], axis=3)
        else:
            ahead = roll_plane(vecf, direction, -1)
            behind = roll_plane(back, direction, 1)
        behind = lax.optimization_barrier(behind).astype(jnp.float32)
        factor = weights[direction].astype(jnp.float32)
        disp = disp + factor * (plain_link(link, ahead) - behind)
    sites = jnp.arange(plane, dtype=jnp.int32)
    xcoord = sites % LX
    ycoord = sites // LX
    zcoord = lax.axis_index("gz") * planes + jnp.arange(planes, dtype=jnp.int32)
    two_pi = 2.0 * math.pi
    inplane = (momentum[0] * xcoord).astype(jnp.float32) / LX + (momentum[1] * ycoord).astype(
        jnp.float32
    ) / LY
    angle = (
        two_pi * inplane[None, :]
        + two_pi * (momentum[2] * zcoord).astype(jnp.float32)[:, None] / depth
    )
    cosine = jnp.cos(angle)
    sine = jnp.sin(angle)
    phased_re = cosine * disp[:, :, 0] + sine * disp[:, :, 1]
    phased_im = cosine * disp[:, :, 1] - sine * disp[:, :, 0]
    phased = jnp.stack([phased_re, phased_im], 2).astype(jnp.bfloat16)
    nsites = planes * plane
    phased = phased.reshape(local_vecs, 3, 2, nsites)
    flat_vecs = eigvec.reshape(local_vecs, 3, 2, nsites)
    scale = 1.0 / math.sqrt(LX * LY * depth)
    blocks = [peram[spins[q, 0], spins[q, 1]] for q in range(3)]
    every = lax.all_gather(flat_vecs, "ea", axis=0, tiled=True)
    count = every.shape[0]
    partial_value = elemental_part(phased, every) * scale
    partial_value = partial_value.reshape(2, local_vecs, count, count)
    partial_value = mode_product(partial_value, blocks[2], "abc,cf->abf")
    partial_value = mode_product(partial_value, blocks[1], "abc,be->aec")
    partial_value = partial_value.reshape(2, local_vecs, count * count)
    summed = lax.psum_scatter(partial_value, "gz", scatter_dimension=2, tiled=True)
    rows = lax.dynamic_slice_in_dim(blocks[0], lax.axis_index("ea") * local_vecs, local_vecs, 1)
    term = mode_product(summed, rows, "ak,ad->dk")
    return lax.psum_scatter(term, "ea", scatter_dimension=1, tiled=True)


def split_dot(coeff, field):
    high = coeff.astype(BF16)
    low = (coeff - high.astype(F32)).astype(BF16)
    return lax.dot_general(high, field, NT, preferred_element_type=F32) + lax.dot_general(
        low, field, NT, preferred_element_type=F32
    )


def shift_x(field, ahead, xcoord):
    size = field.shape[-1]
    if ahead:
        return jnp.where(
            xcoord == LX - 1, pltpu.roll(field, LX - 1, 1), pltpu.roll(field, size - 1, 1)
        )
    return jnp.where(xcoord == 0, pltpu.roll(field, size - LX + 1, 1), pltpu.roll(field, 1, 1))


def shift_y(field, ahead):
    size = field.shape[-1]
    return pltpu.roll(field, size - LX if ahead else LX, 1)


def link_times(links, index, field):
    out = []
    for row in range(3):
        re = im = None
        for col in range(3):
            ur, ui = links(*index, row, col)
            vr, vi = field[col]
            a = ur * vr - ui * vi
            b = ur * vi + ui * vr
            re = a if re is None else re + a
            im = b if im is None else im + b
        out.append((re, im))
    return out


def adjoint_times(links, index, field):
    out = []
    for row in range(3):
        re = im = None
        for col in range(3):
            ur, ui = links(*index, col, row)
            vr, vi = field[col]
            a = ur * vr + ui * vi
            b = ur * vi - ui * vr
            re = a if re is None else re + a
            im = b if im is None else im + b
        out.append((re, im))
    return out


def fields_kernel(weights, phase, links, below, planes, pt0, pt1, pt2, p_ref, v_ref, rhs_ref, u_ref):
    rows0 = pt0.shape[0] // 2
    rows1 = pt1.shape[0] // 2
    rows2 = pt2.shape[0] // 2
    plane = phase.shape[-1]

    def turned(coeff, index, color):
        fr = planes[index, :, pl.ds((2 * color) * plane, plane)]
        fi = planes[index, :, pl.ds((2 * color + 1) * plane, plane)]
        n = coeff.shape[0] // 2
        yr = split_dot(coeff[...], fr)
        yi = split_dot(coeff[...], fi)
        return yr[:n] - yi[n:], yi[:n] + yr[n:]

    for color in range(3):
        for index in range(4):
            re, im = turned(pt0, index, color)
            u_ref[index, 2 * color] = re
            u_ref[index, 2 * color + 1] = im
        for own in range(2):
            at = pl.ds(own * plane, plane)
            re, im = turned(pt1, own + 1, color)
            parts, each = v_ref.shape[1:3]
            for d in range(parts):
                cut = slice(d * each, (d + 1) * each)
                v_ref[3 * color, d, :, at] = re[cut]
                v_ref[3 * color + 1, d, :, at] = im[cut]
                v_ref[3 * color + 2, d, :, at] = re[cut] + im[cut]
            re, im = turned(pt2, own + 1, color)
            re = re.astype(BF16)
            im = im.astype(BF16)
            rhs_ref[2 * color, pl.ds(0, rows2), at] = re
            rhs_ref[2 * color, pl.ds(rows2, rows2), at] = im
            rhs_ref[2 * color + 1, pl.ds(0, rows2), at] = -im
            rhs_ref[2 * color + 1, pl.ds(rows2, rows2), at] = re

    tile = 8
    xcoord = lax.broadcasted_iota(jnp.int32, (tile, plane), 1) % LX

    def one(step, carry):
        rows = pl.ds(pl.multiple_of(step * tile, tile), tile)

        def load(index):
            return [(u_ref[index, 2 * c, rows, :], u_ref[index, 2 * c + 1, rows, :]) for c in range(3)]

        for own in range(2):
            def own_link(direction, row, col, own=own):
                at = ((direction * 3 + row) * 3 + col) * 2
                return links[own, pl.ds(at, 1), :], links[own, pl.ds(at + 1, 1), :]

            def below_link(row, col, own=own):
                if own == 1:
                    return own_link(2, row, col, 0)
                at = (row * 3 + col) * 2
                return below[pl.ds(at, 1), :], below[pl.ds(at + 1, 1), :]

            here = load(own + 1)
            total = [[None, None] for _ in range(3)]
            for direction in range(3):
                back = None
                if direction == 0:
                    ahead = [(shift_x(r, True, xcoord), shift_x(i, True, xcoord)) for r, i in here]
                    back = adjoint_times(own_link, (0,), here)
                    back = [(shift_x(r, False, xcoord), shift_x(i, False, xcoord)) for r, i in back]
                elif direction == 1:
                    ahead = [(shift_y(r, True), shift_y(i, True)) for r, i in here]
                    back = adjoint_times(own_link, (1,), here)
                    back = [(shift_y(r, False), shift_y(i, False)) for r, i in back]
                else:
                    ahead = load(own + 2)
                    back = adjoint_times(below_link, (), load(own))
                front = link_times(own_link, (direction,), ahead)
                factor = weights[direction].astype(F32)
                for k in range(3):
                    for c in range(2):
                        term = factor * (front[k][c] - back[k][c])
                        total[k][c] = term if total[k][c] is None else total[k][c] + term
            cosine = phase[2 * own : 2 * own + 1, :]
            sine = phase[2 * own + 1 : 2 * own + 2, :]
            for k in range(3):
                re = cosine * total[k][0] + sine * total[k][1]
                im = cosine * total[k][1] - sine * total[k][0]
                at = pl.ds(own * plane, plane)
                p_ref[3 * k, rows, at] = re
                p_ref[3 * k + 1, rows, at] = im
                p_ref[3 * k + 2, rows, at] = re + im
        return carry

    lax.fori_loop(0, rows0 // tile, one, 0)


def cross_into(m_ref, p_ref, v_ref, part, count, lanes, width):
    rows = p_ref.shape[1]
    for lane in range(0, width, 128):
        at = pl.ds(pl.multiple_of(lanes + lane, 128), 128)
        for r in range(0, rows, 16):
            p = [p_ref[c, pl.ds(r, 16), at] for c in range(9)]
            for b in range(count):
                v = [v_ref[c, part, pl.ds(b, 1), at] for c in range(9)]
                for j in range(3):
                    k, i = (j + 1) % 3, (j + 2) % 3
                    t = [p[3 * k + s] * v[3 * i + s] - p[3 * i + s] * v[3 * k + s] for s in range(3)]
                    re = t[0] - t[1]
                    im = t[2] - (t[0] + t[1])
                    m_ref[2 * j, pl.ds(b * rows + r, 16), pl.ds(lane, 128)] = re.astype(BF16)
                    m_ref[2 * j + 1, pl.ds(b * rows + r, 16), pl.ds(lane, 128)] = im.astype(BF16)


def contract(m_ref, rhs_ref, lanes, width):
    at = pl.ds(pl.multiple_of(lanes, 128), width)
    total = None
    for j in range(6):
        term = lax.dot_general(
            m_ref[j], rhs_ref[j, :, at], (((1,), (1,)), ((), ())), preferred_element_type=F32
        )
        total = term if total is None else total + term
    return total


def triple_kernel(count, width, p_ref, v_ref, rhs_ref, o_ref, m0, m1):
    sites = p_ref.shape[2]
    chunks = sites // width
    part = pl.program_id(0)
    cross_into(m0, p_ref, v_ref, part, count, 0, width)
    o_ref[0] = jnp.zeros_like(o_ref[0])

    def pair(n, carry):
        lanes = 2 * n * width
        cross_into(m1, p_ref, v_ref, part, count, lanes + width, width)
        o_ref[0] += contract(m0, rhs_ref, lanes, width)
        after = jnp.minimum(lanes + 2 * width, sites - width)
        cross_into(m0, p_ref, v_ref, part, count, after, width)
        o_ref[0] += contract(m1, rhs_ref, lanes + width, width)
        return carry

    lax.fori_loop(0, chunks // 2, pair, 0)


def shards(eigvec, links, momentum, weights, spins, peram):
    local = eigvec.shape[0]
    plane = eigvec.shape[4]
    ndev = lax.axis_size("gz")
    depth = ndev
    me = lax.axis_index("gz")
    odd = me % 2
    own = eigvec.reshape(local, 6 * plane)
    mylinks = links.reshape(54, plane)

    def permute(array, by_even, by_odd):
        moves = [(i, (i + (by_odd if i % 2 else by_even)) % ndev) for i in range(ndev)]
        return lax.ppermute(array, "gz", moves)

    mate = permute(own, 1, -1)
    outer = permute(own, -2, 2)
    cross_outer = permute(own, -1, 1)
    mate_links = permute(mylinks, 1, -1)
    low = jnp.where(odd == 0, own, mate)
    high = jnp.where(odd == 0, mate, own)
    after = jnp.where(odd == 0, outer, cross_outer)
    before = jnp.where(odd == 0, cross_outer, outer)
    planes = jnp.stack([before, low, high, after])
    planes = lax.all_gather(planes, "ea", axis=1, tiled=True)
    low_links = jnp.where(odd == 0, mylinks, mate_links)
    high_links = jnp.where(odd == 0, mate_links, mylinks)
    zlinks = mylinks[36:]
    below = jnp.where(odd == 0, permute(zlinks, -1, 1), permute(zlinks, -2, 2))

    sites = jnp.arange(plane, dtype=jnp.int32)
    zcoord = (me - odd) + jnp.arange(2, dtype=jnp.int32)
    two_pi = 2.0 * math.pi
    inplane = (momentum[0] * (sites % LX)).astype(F32) / LX + (momentum[1] * (sites // LX)).astype(
        F32
    ) / LY
    angle = (
        two_pi * inplane[None, :] + two_pi * (momentum[2] * zcoord).astype(F32)[:, None] / depth
    )
    scale = 1.0 / math.sqrt(plane * depth)
    phase = (jnp.stack([jnp.cos(angle), jnp.sin(angle)], 1) * scale).reshape(4, plane)

    blocks = [peram[spins[q, 0], spins[q, 1]] for q in range(3)]
    count = blocks[0].shape[1]
    each = count // ndev
    half = ndev // 2
    pt0 = lax.dynamic_slice_in_dim(blocks[0], lax.axis_index("ea") * local, local, 2)
    pt1 = blocks[1].reshape(2, count, half, 2, each)
    pt1 = lax.dynamic_index_in_dim(pt1, odd, 3, False).reshape(2, count, half * each)
    turn = lambda x: x.transpose(0, 2, 1).reshape(-1, count)
    vmem = pl.BlockSpec(memory_space=pltpu.VMEM)
    total = 2 * plane
    params = pltpu.CompilerParams(vmem_limit_bytes=60 * 1024 * 1024)
    p, v, rhs = pl.pallas_call(
        fields_kernel,
        out_shape=(
            jax.ShapeDtypeStruct((9, local, total), F32),
            jax.ShapeDtypeStruct((9, half, each, total), F32),
            jax.ShapeDtypeStruct((6, 2 * count, total), BF16),
        ),
        in_specs=[pl.BlockSpec(memory_space=pltpu.SMEM)] + [vmem] * 7,
        out_specs=(vmem, vmem, vmem),
        scratch_shapes=[pltpu.VMEM((4, 6, local, plane), F32)],
        compiler_params=params,
        name="fields",
    )(
        weights,
        phase,
        jnp.stack([low_links, high_links]),
        below,
        planes,
        turn(pt0),
        turn(pt1),
        turn(blocks[2]),
    )
    width = 256
    out = pl.pallas_call(
        functools.partial(triple_kernel, each, width),
        grid=(half,),
        out_shape=jax.ShapeDtypeStruct((half, each * local, 2 * count), F32),
        in_specs=[vmem] * 3,
        out_specs=pl.BlockSpec((1, each * local, 2 * count), lambda d: (d, 0, 0)),
        scratch_shapes=[pltpu.VMEM((6, each * local, width), BF16) for _ in range(2)],
        compiler_params=params,
        name="triple",
    )(p, v, rhs)
    groups = [[i for i in range(ndev) if i % 2 == par] for par in range(2)]
    got = lax.all_to_all(
        out.astype(BF16), "gz", 0, 0, axis_index_groups=groups, tiled=True
    )
    got = lax.optimization_barrier(got)
    total_out = jnp.sum(got.astype(F32), 0)
    total_out = total_out.reshape(each, local, 2, count).transpose(2, 1, 0, 3)
    return total_out.reshape(2, local, each * count)


def solution(mesh):
    ndev = mesh.shape["gz"]
    in_specs = (
        P("ea", None, None, ("groups", "gz"), None),
        P(None, None, None, None, ("groups", "gz"), None),
        P("groups"),
        P("groups"),
        P("groups", None),
        P("groups", None, None, None, None),
    )
    out_specs = P("groups", "ea", "gz")

    def body(eigvec, links, momentum, weights, spins, peram):
        whole_rows = peram.shape[-1] % ndev == 0 and ndev % 2 == 0 and eigvec.shape[3] == 1
        run = shards if whole_rows else plain_shards
        return run(eigvec, links, momentum, weights, spins, peram)

    return jax.shard_map(body, mesh=mesh, in_specs=in_specs, out_specs=out_specs, check_vma=False)
```

```python
import functools
import math

import jax
import jax.numpy as jnp
from jax import lax
from jax.experimental import pallas as pl
from jax.experimental.pallas import tpu as pltpu
from jax.sharding import PartitionSpec as P

LX = 32
LY = 16
F32 = jnp.float32
BF16 = jnp.bfloat16
NT = (((1,), (0,)), ((), ()))


def from_behind(array, axis, by):
    count = lax.axis_size(axis)
    return lax.ppermute(array, axis, [(i, (i + by) % count) for i in range(count)])


def plain_link(link, lattice_field):
    result_real = 0.0
    result_imaginary = 0.0
    for column_slot in range(3):
        gauge_link_real = link[None, :, column_slot, 0]
        gauge_link_imaginary = link[None, :, column_slot, 1]
        vector_real = lattice_field[:, None, column_slot, 0]
        vector_imaginary = lattice_field[:, None, column_slot, 1]
        result_real = (
            result_real + gauge_link_real * vector_real - gauge_link_imaginary * vector_imaginary
        )
        result_imaginary = (
            result_imaginary
            + gauge_link_real * vector_imaginary
            + gauge_link_imaginary * vector_real
        )
    return jnp.stack([result_real, result_imaginary], 2)


def adjoint_apply(link, lattice_field):
    result_real = 0.0
    result_imaginary = 0.0
    for column_slot in range(3):
        gauge_link_real = link[None, column_slot, :, 0]
        gauge_link_imaginary = link[None, column_slot, :, 1]
        vector_real = lattice_field[:, None, column_slot, 0]
        vector_imaginary = lattice_field[:, None, column_slot, 1]
        result_real = (
            result_real + gauge_link_real * vector_real + gauge_link_imaginary * vector_imaginary
        )
        result_imaginary = (
            result_imaginary
            + gauge_link_real * vector_imaginary
            - gauge_link_imaginary * vector_real
        )
    return jnp.stack([result_real, result_imaginary], 2)


def cross_parts(left_vec, right_vec):
    reals = []
    imags = []
    for first, second in ((1, 2), (2, 0), (0, 1)):
        ar = left_vec[:, :, first, 0]
        ai = left_vec[:, :, first, 1]
        br = left_vec[:, :, second, 0]
        bi = left_vec[:, :, second, 1]
        cr = right_vec[:, :, first, 0]
        ci = right_vec[:, :, first, 1]
        dr = right_vec[:, :, second, 0]
        di = right_vec[:, :, second, 1]
        reals.append(ar * dr - ai * di - (br * cr - bi * ci))
        imags.append(ar * di + ai * dr - (br * ci + bi * cr))
    return jnp.stack([jnp.stack(reals), jnp.stack(imags)])


def mode_product(lattice_field, block, form):
    high = lax.Precision.HIGHEST
    real_part = jnp.einsum(form, lattice_field[0], block[0], precision=high) - jnp.einsum(
        form, lattice_field[1], block[1], precision=high
    )
    imag_part = jnp.einsum(form, lattice_field[0], block[1], precision=high) + jnp.einsum(
        form, lattice_field[1], block[0], precision=high
    )
    return jnp.stack([real_part, imag_part])


def roll_plane(lattice_field, direction, amount):
    grid = lattice_field.reshape(lattice_field.shape[:-1] + (LY, LX))
    axis_here = grid.ndim - 1 if direction == 0 else grid.ndim - 2
    return jnp.roll(grid, amount, axis_here).reshape(lattice_field.shape)


def elemental_part(phased, vectors):
    count = vectors.shape[0]
    size_a = phased.shape[0]
    nsites = vectors.shape[3]
    real_part = phased[:, :, 0]
    imag_part = phased[:, :, 1]
    upper_rows = jnp.stack([real_part, -imag_part], 1)
    lower_rows = jnp.stack([imag_part, real_part], 1)
    left = jnp.stack([upper_rows, lower_rows], 0).reshape(2 * size_a, 2, 3, nsites)
    width = min(8, count)
    others = vectors.astype(jnp.float32)[None]

    def one_block(rows):
        wmat = cross_parts(rows.astype(jnp.float32)[:, None], others).astype(jnp.bfloat16)
        return jnp.einsum("xrks,rkbcs->xbc", left, wmat, preferred_element_type=jnp.float32)

    result = lax.map(one_block, vectors.reshape(count // width, width, 3, 2, nsites))
    return result.transpose(1, 0, 2, 3).reshape(2, size_a, count * count)


def plain_shards(eigvec, links, momentum, weights, spins, peram):
    local_vecs = eigvec.shape[0]
    planes = eigvec.shape[3]
    plane = eigvec.shape[4]
    depth = planes * lax.axis_size("gz")
    vecf = eigvec.astype(jnp.float32)
    disp = jnp.zeros(vecf.shape, jnp.float32)
    for direction in range(3):
        link = links[direction]
        back = adjoint_apply(link, vecf).astype(jnp.bfloat16)
        if direction == 2:
            upper = from_behind(eigvec, "gz", -1)
            ahead = jnp.concatenate([eigvec[:, :, :, 1:], upper], axis=3).astype(jnp.float32)
            lower = from_behind(back, "gz", 1)
            behind = jnp.concatenate([lower, back[:, :, :, :-1]], axis=3)
        else:
            ahead = roll_plane(vecf, direction, -1)
            behind = roll_plane(back, direction, 1)
        behind = lax.optimization_barrier(behind).astype(jnp.float32)
        factor = weights[direction].astype(jnp.float32)
        disp = disp + factor * (plain_link(link, ahead) - behind)
    sites = jnp.arange(plane, dtype=jnp.int32)
    xcoord = sites % LX
    ycoord = sites // LX
    zcoord = lax.axis_index("gz") * planes + jnp.arange(planes, dtype=jnp.int32)
    two_pi = 2.0 * math.pi
    inplane = (momentum[0] * xcoord).astype(jnp.float32) / LX + (momentum[1] * ycoord).astype(
        jnp.float32
    ) / LY
    angle = (
        two_pi * inplane[None, :]
        + two_pi * (momentum[2] * zcoord).astype(jnp.float32)[:, None] / depth
    )
    cosine = jnp.cos(angle)
    sine = jnp.sin(angle)
    phased_re = cosine * disp[:, :, 0] + sine * disp[:, :, 1]
    phased_im = cosine * disp[:, :, 1] - sine * disp[:, :, 0]
    phased = jnp.stack([phased_re, phased_im], 2).astype(jnp.bfloat16)
    nsites = planes * plane
    phased = phased.reshape(local_vecs, 3, 2, nsites)
    flat_vecs = eigvec.reshape(local_vecs, 3, 2, nsites)
    scale = 1.0 / math.sqrt(LX * LY * depth)
    blocks = [peram[spins[q, 0], spins[q, 1]] for q in range(3)]
    every = lax.all_gather(flat_vecs, "ea", axis=0, tiled=True)
    count = every.shape[0]
    partial_value = elemental_part(phased, every) * scale
    partial_value = partial_value.reshape(2, local_vecs, count, count)
    partial_value = mode_product(partial_value, blocks[2], "abc,cf->abf")
    partial_value = mode_product(partial_value, blocks[1], "abc,be->aec")
    partial_value = partial_value.reshape(2, local_vecs, count * count)
    summed = lax.psum_scatter(partial_value, "gz", scatter_dimension=2, tiled=True)
    rows = lax.dynamic_slice_in_dim(blocks[0], lax.axis_index("ea") * local_vecs, local_vecs, 1)
    term = mode_product(summed, rows, "ak,ad->dk")
    return lax.psum_scatter(term, "ea", scatter_dimension=1, tiled=True)


def split_dot(coeff, field):
    high = coeff.astype(BF16)
    low = (coeff - high.astype(F32)).astype(BF16)
    return lax.dot_general(high, field, NT, preferred_element_type=F32) + lax.dot_general(
        low, field, NT, preferred_element_type=F32
    )


def shift_x(field, ahead, xcoord):
    size = field.shape[-1]
    if ahead:
        return jnp.where(
            xcoord == LX - 1, pltpu.roll(field, LX - 1, 1), pltpu.roll(field, size - 1, 1)
        )
    return jnp.where(xcoord == 0, pltpu.roll(field, size - LX + 1, 1), pltpu.roll(field, 1, 1))


def shift_y(field, ahead):
    size = field.shape[-1]
    return pltpu.roll(field, size - LX if ahead else LX, 1)


def link_times(links, index, field):
    out = []
    for row in range(3):
        re = im = None
        for col in range(3):
            ur, ui = links(*index, row, col)
            vr, vi = field[col]
            a = ur * vr - ui * vi
            b = ur * vi + ui * vr
            re = a if re is None else re + a
            im = b if im is None else im + b
        out.append((re, im))
    return out


def adjoint_times(links, index, field):
    out = []
    for row in range(3):
        re = im = None
        for col in range(3):
            ur, ui = links(*index, col, row)
            vr, vi = field[col]
            a = ur * vr + ui * vi
            b = ur * vi - ui * vr
            re = a if re is None else re + a
            im = b if im is None else im + b
        out.append((re, im))
    return out


def fill_fields(slot, pair, planes, pts, first_row, parity, u_ref, v_ref, rhs_ref, plane):
    rows0 = u_ref.shape[2]
    count = pts.shape[2]

    def turned(which, rows, color):
        fr = planes[slot, :, pl.ds((2 * color) * plane, plane)]
        fi = planes[slot, :, pl.ds((2 * color + 1) * plane, plane)]
        coeff = jnp.concatenate([rows(which, 0), rows(which, 1)], 0)
        n = coeff.shape[0] // 2
        yr = split_dot(coeff, fr)
        yi = split_dot(coeff, fi)
        return yr[:n] - yi[n:], yi[:n] + yr[n:]

    def own_rows(which, part):
        return pts[which, part, pl.ds(first_row, rows0), :]

    def all_rows(which, part):
        return pts[which, part]

    for color in range(3):
        re, im = turned(0, own_rows, color)
        u_ref[slot, 2 * color] = re
        u_ref[slot, 2 * color + 1] = im
        if not pair:
            continue
        at = pl.ds(pl.multiple_of((slot - 1) * plane, plane), plane)
        parts, each = v_ref.shape[1:3]
        re, im = turned(1, all_rows, color)
        for d in range(parts):
            low = slice(2 * d * each, (2 * d + 1) * each)
            high = slice((2 * d + 1) * each, (2 * d + 2) * each)
            vr = jnp.where(parity == 0, re[low], re[high])
            vi = jnp.where(parity == 0, im[low], im[high])
            v_ref[3 * color, d, :, at] = vr
            v_ref[3 * color + 1, d, :, at] = vi
            v_ref[3 * color + 2, d, :, at] = vr + vi
        re, im = turned(2, all_rows, color)
        re = re.astype(BF16)
        im = im.astype(BF16)
        rhs_ref[2 * color, pl.ds(0, count), at] = re
        rhs_ref[2 * color, pl.ds(count, count), at] = im
        rhs_ref[2 * color + 1, pl.ds(0, count), at] = -im
        rhs_ref[2 * color + 1, pl.ds(count, count), at] = re


def displace(weights, phases, links, below, u_ref, p_ref, plane):
    tile = 8
    xcoord = lax.broadcasted_iota(jnp.int32, (tile, plane), 1) % LX

    def one(step, carry):
        rows = pl.ds(pl.multiple_of(step * tile, tile), tile)

        def load(index):
            return [(u_ref[index, 2 * c, rows, :], u_ref[index, 2 * c + 1, rows, :]) for c in range(3)]

        for own in range(2):
            def own_link(direction, row, col, own=own):
                at = ((direction * 3 + row) * 3 + col) * 2
                return links[own, pl.ds(at, 1), :], links[own, pl.ds(at + 1, 1), :]

            def below_link(row, col, own=own):
                if own == 1:
                    return own_link(2, row, col, 0)
                at = (row * 3 + col) * 2
                return below[pl.ds(at, 1), :], below[pl.ds(at + 1, 1), :]

            here = load(own + 1)
            total = [[None, None] for _ in range(3)]
            for direction in range(3):
                if direction == 0:
                    ahead = [(shift_x(r, True, xcoord), shift_x(i, True, xcoord)) for r, i in here]
                    back = adjoint_times(own_link, (0,), here)
                    back = [(shift_x(r, False, xcoord), shift_x(i, False, xcoord)) for r, i in back]
                elif direction == 1:
                    ahead = [(shift_y(r, True), shift_y(i, True)) for r, i in here]
                    back = adjoint_times(own_link, (1,), here)
                    back = [(shift_y(r, False), shift_y(i, False)) for r, i in back]
                else:
                    ahead = load(own + 2)
                    back = adjoint_times(below_link, (), load(own))
                front = link_times(own_link, (direction,), ahead)
                factor = weights[direction].astype(F32)
                for k in range(3):
                    for c in range(2):
                        term = factor * (front[k][c] - back[k][c])
                        total[k][c] = term if total[k][c] is None else total[k][c] + term
            cosine, sine = phases[own]
            at = pl.ds(own * plane, plane)
            for k in range(3):
                re = cosine * total[k][0] + sine * total[k][1]
                im = cosine * total[k][1] - sine * total[k][0]
                p_ref[3 * k, rows, at] = re
                p_ref[3 * k + 1, rows, at] = im
                p_ref[3 * k + 2, rows, at] = re + im
        return carry

    lax.fori_loop(0, p_ref.shape[1] // tile, one, 0)


def cross_tile(m_ref, p_ref, v_ref, part, lanes, lane, r):
    rows = p_ref.shape[1]
    at = pl.ds(pl.multiple_of(lanes + lane, 128), 128)
    p = [p_ref[c, pl.ds(r, 16), at] for c in range(9)]
    for b in range(v_ref.shape[2]):
        v = [v_ref[c, part, pl.ds(b, 1), at] for c in range(9)]
        to = pl.ds(pl.multiple_of(b * rows + r, 16), 16)
        for j in range(3):
            k, i = (j + 1) % 3, (j + 2) % 3
            t = [p[3 * k + s] * v[3 * i + s] - p[3 * i + s] * v[3 * k + s] for s in range(3)]
            re = t[0] - t[1]
            im = t[2] - (t[0] + t[1])
            m_ref[2 * j, to, pl.ds(lane, 128)] = re.astype(BF16)
            m_ref[2 * j + 1, to, pl.ds(lane, 128)] = im.astype(BF16)


def mixed(next_ref, now_ref, p_ref, v_ref, rhs_ref, acc, part, lanes, now_lanes, now_first):
    width = next_ref.shape[2]
    rows = p_ref.shape[1]
    at = pl.ds(pl.multiple_of(now_lanes, 128), width)

    def body(t, carry):
        r = pl.multiple_of(t * 16, 16)
        for lane in range(0, width, 128):
            cross_tile(next_ref, p_ref, v_ref, part, lanes, lane, r)
        total = None
        for j in range(2):
            term = lax.dot_general(
                now_ref[2 * t + j],
                rhs_ref[2 * t + j, :, at],
                (((1,), (1,)), ((), ())),
                preferred_element_type=F32,
            )
            total = term if total is None else total + term
        keep = jnp.where(jnp.logical_and(now_first, t == 0), 0.0, 1.0)
        acc[...] = acc[...] * keep + total
        return carry

    lax.fori_loop(0, 3, body, 0)


def block_kernel(names, weights, momentum, own_ref, links_ref, zlinks_ref, pts, o_ref, planes, links,
                 below, u_ref, p_ref, v_ref, rhs_ref, acc, m0, m1, stage, arrived, psend, precv, ssend,
                 srecv, lsend, lrecv, bsend, brecv, rsend, rrecv):
    gz, ea, ndev = names
    me = lax.axis_index(gz)
    core = lax.axis_index(ea)
    odd = me % 2
    half = ndev // 2
    local, width6 = own_ref.shape
    plane = width6 // 6

    def at_gz(index):
        return {gz: index}

    sibling = {ea: 1 - core}
    mate = me + 1 - 2 * odd
    side = lax.rem(me + ndev - 1 + 2 * odd, ndev)
    jump = lax.rem(me + ndev - 2 + 4 * odd, ndev)

    def same_parity(t):
        return lax.rem(me + 2 * t, ndev)

    barrier = pltpu.get_barrier_semaphore()
    friends = [sibling, at_gz(mate), at_gz(side)] + [at_gz(same_parity(t)) for t in range(1, half)]
    for friend in friends:
        pl.semaphore_signal(barrier, inc=1, device_id=friend, device_id_type=pl.DeviceIdType.MESH)
    pl.semaphore_wait(barrier, len(friends))

    mine = pl.ds(pl.multiple_of(core * local, 16), local)
    my_slot = 1 + odd
    mate_slot = 2 - odd
    out_slot = 3 - 3 * odd

    def remote(src, dst, send, recv, device):
        return pltpu.make_async_remote_copy(
            src_ref=src, dst_ref=dst, send_sem=send, recv_sem=recv, device_id=device,
            device_id_type=pl.DeviceIdType.MESH,
        )

    share = remote(own_ref, planes.at[my_slot, mine], ssend.at[my_slot], srecv.at[my_slot], sibling)
    share.start()
    to_mate = remote(own_ref, planes.at[my_slot, mine], psend.at[0], precv.at[my_slot], at_gz(mate))
    to_mate.start()
    to_side = remote(own_ref, planes.at[out_slot, mine], psend.at[1], precv.at[out_slot], at_gz(side))
    to_jump = remote(own_ref, planes.at[out_slot, mine], psend.at[2], precv.at[out_slot], at_gz(jump))
    to_side.start()
    to_jump.start()
    link_mate = remote(links_ref, links.at[odd], lsend, lrecv.at[odd], at_gz(mate))
    link_mate.start()
    z_side = remote(zlinks_ref, below, bsend.at[0], brecv, at_gz(side))
    z_jump = remote(zlinks_ref, below, bsend.at[1], brecv, at_gz(jump))

    @pl.when(odd == 1)
    def _():
        z_side.start()
        z_jump.start()

    planes[my_slot, mine, :] = own_ref[...]
    links[odd] = links_ref[...]

    def landed(slot, recv):
        return remote(own_ref, planes.at[slot, mine], psend.at[0], recv.at[slot], sibling)

    def fill(slot, pair):
        fill_fields(slot, pair, planes, pts, pl.multiple_of(core * local, 8), odd, u_ref, v_ref,
                    rhs_ref, plane)

    def theirs(slot):
        rows = pl.ds(pl.multiple_of((1 - core) * local, 16), local)
        return remote(own_ref, planes.at[slot, rows], psend.at[0], srecv.at[slot], sibling)

    theirs(my_slot).wait_recv()
    fill(my_slot, True)
    for slot, pair in ((mate_slot, True), (0, False), (3, False)):
        landed(slot, precv).wait_recv()
        block = planes.at[slot, mine]
        remote(block, block, ssend.at[slot], srecv.at[slot], sibling).start()
        theirs(slot).wait_recv()
        fill(slot, pair)
    remote(links_ref, links.at[1 - odd], lsend, lrecv.at[1 - odd], at_gz(mate)).wait_recv()
    z_side.wait_recv()

    sites = lax.broadcasted_iota(jnp.int32, (1, plane), 1)
    two_pi = 2.0 * math.pi
    scale = 1.0 / math.sqrt(plane * ndev)
    inplane = (momentum[0] * (sites % LX)).astype(F32) / LX + (
        momentum[1] * (sites // LX)
    ).astype(F32) / LY
    phases = []
    for own in range(2):
        height = jnp.full((1, plane), momentum[2] * (me - odd + own), jnp.int32).astype(F32)
        angle = two_pi * inplane + two_pi * height / ndev
        phases.append((jnp.cos(angle) * scale, jnp.sin(angle) * scale))
    displace(weights, phases, links, below, u_ref, p_ref, plane)

    width = m0.shape[2]
    chunks = p_ref.shape[2] // width
    total = half * chunks
    zplace = me // 2

    def place(n):
        return lax.rem(zplace + 1 + n // chunks, half), (n % chunks) * width

    part, lanes = place(0)

    def begin(t, carry):
        for lane in range(0, width, 128):
            cross_tile(m0, p_ref, v_ref, part, lanes, lane, pl.multiple_of(t * 16, 16))
        return carry

    lax.fori_loop(0, 3, begin, 0)
    short = acc.shape[0] // 2
    wide = acc.shape[1]

    def send(t):
        return remote(stage.at[t], arrived.at[t], rsend.at[t], rrecv.at[t], at_gz(same_parity(t + 1)))

    def stretch(n, carry):
        for sub, (now, after) in enumerate(((m0, m1), (m1, m0))):
            step = 2 * n + sub
            now_part, now_lanes = place(step)
            part, lanes = place(jnp.minimum(step + 1, total - 1))
            mixed(after, now, p_ref, v_ref, rhs_ref, acc, part, lanes, now_lanes, step % chunks == 0)
        return carry

    def one_part(d, carry):
        lax.fori_loop(d * (chunks // 2), (d + 1) * (chunks // 2), stretch, 0)

        @pl.when(d < half - 1)
        def _():
            stage[d, :, pl.ds(0, wide)] = acc[pl.ds(0, short), :].astype(BF16)
            stage[d, :, pl.ds(wide, wide)] = acc[pl.ds(short, short), :].astype(BF16)
            send(d).start()

        return carry

    lax.fori_loop(0, half, one_part, 0)
    o_ref[:, pl.ds(0, wide)] = acc[pl.ds(0, short), :]
    o_ref[:, pl.ds(wide, wide)] = acc[pl.ds(short, short), :]
    for t in range(half - 1):
        send(t).wait_recv()
        o_ref[...] += arrived[t].astype(F32)
    for t in range(half - 1):
        send(t).wait_send()
    to_mate.wait_send()
    to_side.wait_send()
    to_jump.wait_send()
    link_mate.wait_send()
    for slot in range(4):
        block = planes.at[slot, mine]
        remote(block, block, ssend.at[slot], srecv.at[slot], sibling).wait_send()

    @pl.when(odd == 1)
    def _():
        z_side.wait_send()
        z_jump.wait_send()


def shards(eigvec, links, momentum, weights, spins, peram):
    local = eigvec.shape[0]
    plane = eigvec.shape[4]
    ndev = lax.axis_size("gz")
    count = peram.shape[-1]
    each = count // ndev
    half = ndev // 2
    own = eigvec.reshape(local, 6 * plane)
    mylinks = links.reshape(54, plane)
    pts = jnp.stack([peram[spins[q, 0], spins[q, 1]] for q in range(3)]).swapaxes(2, 3)
    vmem = pl.BlockSpec(memory_space=pltpu.VMEM)
    smem = pl.BlockSpec(memory_space=pltpu.SMEM)
    total = 2 * plane
    width = 256
    rows = each * local
    dma = pltpu.SemaphoreType.DMA
    out = pl.pallas_call(
        functools.partial(block_kernel, ("gz", "ea", ndev)),
        out_shape=jax.ShapeDtypeStruct((rows // 2, 4 * count), F32),
        in_specs=[smem, smem, vmem, vmem, vmem, vmem],
        out_specs=vmem,
        scratch_shapes=[
            pltpu.VMEM((4, 2 * local, 6 * plane), BF16),
            pltpu.VMEM((2, 54, plane), F32),
            pltpu.VMEM((18, plane), F32),
            pltpu.VMEM((4, 6, local, plane), F32),
            pltpu.VMEM((9, local, total), F32),
            pltpu.VMEM((9, half, each, total), F32),
            pltpu.VMEM((6, 2 * count, total), BF16),
            pltpu.VMEM((rows, 2 * count), F32),
            pltpu.VMEM((6, rows, width), BF16),
            pltpu.VMEM((6, rows, width), BF16),
            pltpu.VMEM((half - 1, rows // 2, 4 * count), BF16),
            pltpu.VMEM((half - 1, rows // 2, 4 * count), BF16),
            dma((3,)),
            dma((4,)),
            dma((4,)),
            dma((4,)),
            dma,
            dma((2,)),
            dma((2,)),
            dma,
            dma((half - 1,)),
            dma((half - 1,)),
        ],
        compiler_params=pltpu.CompilerParams(
            vmem_limit_bytes=62 * 1024 * 1024, collective_id=0, has_side_effects=True
        ),
        name="block",
    )(weights, momentum, own, mylinks, mylinks[36:], pts)
    out = out.reshape(each // 2, local, 2, 2, count).transpose(3, 1, 2, 0, 4)
    return out.reshape(2, local, each * count)


def solution(mesh):
    ndev = mesh.shape["gz"]
    in_specs = (
        P("ea", None, None, ("groups", "gz"), None),
        P(None, None, None, None, ("groups", "gz"), None),
        P("groups"),
        P("groups"),
        P("groups", None),
        P("groups", None, None, None, None),
    )
    out_specs = P("groups", "ea", "gz")

    def body(eigvec, links, momentum, weights, spins, peram):
        whole_rows = peram.shape[-1] % (2 * ndev) == 0 and ndev % 2 == 0 and ndev > 2
        whole_rows = whole_rows and eigvec.shape[3] == 1
        run = shards if whole_rows else plain_shards
        return run(eigvec, links, momentum, weights, spins, peram)

    return jax.shard_map(body, mesh=mesh, in_specs=in_specs, out_specs=out_specs, check_vma=False)
```

```python
import functools
import math

import jax
import jax.numpy as jnp
from jax import lax
from jax.experimental import pallas as pl
from jax.experimental.pallas import tpu as pltpu
from jax.sharding import PartitionSpec as P

LX = 32
LY = 16
F32 = jnp.float32
BF16 = jnp.bfloat16
NT = (((1,), (0,)), ((), ()))


def from_behind(array, axis, by):
    count = lax.axis_size(axis)
    return lax.ppermute(array, axis, [(i, (i + by) % count) for i in range(count)])


def plain_link(link, lattice_field):
    result_real = 0.0
    result_imaginary = 0.0
    for column_slot in range(3):
        gauge_link_real = link[None, :, column_slot, 0]
        gauge_link_imaginary = link[None, :, column_slot, 1]
        vector_real = lattice_field[:, None, column_slot, 0]
        vector_imaginary = lattice_field[:, None, column_slot, 1]
        result_real = (
            result_real + gauge_link_real * vector_real - gauge_link_imaginary * vector_imaginary
        )
        result_imaginary = (
            result_imaginary
            + gauge_link_real * vector_imaginary
            + gauge_link_imaginary * vector_real
        )
    return jnp.stack([result_real, result_imaginary], 2)


def adjoint_apply(link, lattice_field):
    result_real = 0.0
    result_imaginary = 0.0
    for column_slot in range(3):
        gauge_link_real = link[None, column_slot, :, 0]
        gauge_link_imaginary = link[None, column_slot, :, 1]
        vector_real = lattice_field[:, None, column_slot, 0]
        vector_imaginary = lattice_field[:, None, column_slot, 1]
        result_real = (
            result_real + gauge_link_real * vector_real + gauge_link_imaginary * vector_imaginary
        )
        result_imaginary = (
            result_imaginary
            + gauge_link_real * vector_imaginary
            - gauge_link_imaginary * vector_real
        )
    return jnp.stack([result_real, result_imaginary], 2)


def cross_parts(left_vec, right_vec):
    reals = []
    imags = []
    for first, second in ((1, 2), (2, 0), (0, 1)):
        ar = left_vec[:, :, first, 0]
        ai = left_vec[:, :, first, 1]
        br = left_vec[:, :, second, 0]
        bi = left_vec[:, :, second, 1]
        cr = right_vec[:, :, first, 0]
        ci = right_vec[:, :, first, 1]
        dr = right_vec[:, :, second, 0]
        di = right_vec[:, :, second, 1]
        reals.append(ar * dr - ai * di - (br * cr - bi * ci))
        imags.append(ar * di + ai * dr - (br * ci + bi * cr))
    return jnp.stack([jnp.stack(reals), jnp.stack(imags)])


def mode_product(lattice_field, block, form):
    high = lax.Precision.HIGHEST
    real_part = jnp.einsum(form, lattice_field[0], block[0], precision=high) - jnp.einsum(
        form, lattice_field[1], block[1], precision=high
    )
    imag_part = jnp.einsum(form, lattice_field[0], block[1], precision=high) + jnp.einsum(
        form, lattice_field[1], block[0], precision=high
    )
    return jnp.stack([real_part, imag_part])


def roll_plane(lattice_field, direction, amount):
    grid = lattice_field.reshape(lattice_field.shape[:-1] + (LY, LX))
    axis_here = grid.ndim - 1 if direction == 0 else grid.ndim - 2
    return jnp.roll(grid, amount, axis_here).reshape(lattice_field.shape)


def elemental_part(phased, vectors):
    count = vectors.shape[0]
    size_a = phased.shape[0]
    nsites = vectors.shape[3]
    real_part = phased[:, :, 0]
    imag_part = phased[:, :, 1]
    upper_rows = jnp.stack([real_part, -imag_part], 1)
    lower_rows = jnp.stack([imag_part, real_part], 1)
    left = jnp.stack([upper_rows, lower_rows], 0).reshape(2 * size_a, 2, 3, nsites)
    width = min(8, count)
    others = vectors.astype(jnp.float32)[None]

    def one_block(rows):
        wmat = cross_parts(rows.astype(jnp.float32)[:, None], others).astype(jnp.bfloat16)
        return jnp.einsum("xrks,rkbcs->xbc", left, wmat, preferred_element_type=jnp.float32)

    result = lax.map(one_block, vectors.reshape(count // width, width, 3, 2, nsites))
    return result.transpose(1, 0, 2, 3).reshape(2, size_a, count * count)


def plain_shards(eigvec, links, momentum, weights, spins, peram):
    local_vecs = eigvec.shape[0]
    planes = eigvec.shape[3]
    plane = eigvec.shape[4]
    depth = planes * lax.axis_size("gz")
    vecf = eigvec.astype(jnp.float32)
    disp = jnp.zeros(vecf.shape, jnp.float32)
    for direction in range(3):
        link = links[direction]
        back = adjoint_apply(link, vecf).astype(jnp.bfloat16)
        if direction == 2:
            upper = from_behind(eigvec, "gz", -1)
            ahead = jnp.concatenate([eigvec[:, :, :, 1:], upper], axis=3).astype(jnp.float32)
            lower = from_behind(back, "gz", 1)
            behind = jnp.concatenate([lower, back[:, :, :, :-1]], axis=3)
        else:
            ahead = roll_plane(vecf, direction, -1)
            behind = roll_plane(back, direction, 1)
        behind = lax.optimization_barrier(behind).astype(jnp.float32)
        factor = weights[direction].astype(jnp.float32)
        disp = disp + factor * (plain_link(link, ahead) - behind)
    sites = jnp.arange(plane, dtype=jnp.int32)
    xcoord = sites % LX
    ycoord = sites // LX
    zcoord = lax.axis_index("gz") * planes + jnp.arange(planes, dtype=jnp.int32)
    two_pi = 2.0 * math.pi
    inplane = (momentum[0] * xcoord).astype(jnp.float32) / LX + (momentum[1] * ycoord).astype(
        jnp.float32
    ) / LY
    angle = (
        two_pi * inplane[None, :]
        + two_pi * (momentum[2] * zcoord).astype(jnp.float32)[:, None] / depth
    )
    cosine = jnp.cos(angle)
    sine = jnp.sin(angle)
    phased_re = cosine * disp[:, :, 0] + sine * disp[:, :, 1]
    phased_im = cosine * disp[:, :, 1] - sine * disp[:, :, 0]
    phased = jnp.stack([phased_re, phased_im], 2).astype(jnp.bfloat16)
    nsites = planes * plane
    phased = phased.reshape(local_vecs, 3, 2, nsites)
    flat_vecs = eigvec.reshape(local_vecs, 3, 2, nsites)
    scale = 1.0 / math.sqrt(LX * LY * depth)
    blocks = [peram[spins[q, 0], spins[q, 1]] for q in range(3)]
    every = lax.all_gather(flat_vecs, "ea", axis=0, tiled=True)
    count = every.shape[0]
    partial_value = elemental_part(phased, every) * scale
    partial_value = partial_value.reshape(2, local_vecs, count, count)
    partial_value = mode_product(partial_value, blocks[2], "abc,cf->abf")
    partial_value = mode_product(partial_value, blocks[1], "abc,be->aec")
    partial_value = partial_value.reshape(2, local_vecs, count * count)
    summed = lax.psum_scatter(partial_value, "gz", scatter_dimension=2, tiled=True)
    rows = lax.dynamic_slice_in_dim(blocks[0], lax.axis_index("ea") * local_vecs, local_vecs, 1)
    term = mode_product(summed, rows, "ak,ad->dk")
    return lax.psum_scatter(term, "ea", scatter_dimension=1, tiled=True)


def split_dot(coeff, field):
    high = coeff.astype(BF16)
    low = (coeff - high.astype(F32)).astype(BF16)
    return lax.dot_general(high, field, NT, preferred_element_type=F32) + lax.dot_general(
        low, field, NT, preferred_element_type=F32
    )


def shift_x(field, ahead, xcoord):
    size = field.shape[-1]
    if ahead:
        return jnp.where(
            xcoord == LX - 1, pltpu.roll(field, LX - 1, 1), pltpu.roll(field, size - 1, 1)
        )
    return jnp.where(xcoord == 0, pltpu.roll(field, size - LX + 1, 1), pltpu.roll(field, 1, 1))


def shift_y(field, ahead):
    size = field.shape[-1]
    return pltpu.roll(field, size - LX if ahead else LX, 1)


def link_times(links, index, field):
    out = []
    for row in range(3):
        re = im = None
        for col in range(3):
            ur, ui = links(*index, row, col)
            vr, vi = field[col]
            a = ur * vr - ui * vi
            b = ur * vi + ui * vr
            re = a if re is None else re + a
            im = b if im is None else im + b
        out.append((re, im))
    return out


def adjoint_times(links, index, field):
    out = []
    for row in range(3):
        re = im = None
        for col in range(3):
            ur, ui = links(*index, col, row)
            vr, vi = field[col]
            a = ur * vr + ui * vi
            b = ur * vi - ui * vr
            re = a if re is None else re + a
            im = b if im is None else im + b
        out.append((re, im))
    return out


def fill_fields(slot, pair, planes, pts, first_row, parity, u_ref, v_ref, rhs_ref, plane):
    rows0 = u_ref.shape[2]
    count = pts.shape[2]

    def turned(which, rows, color):
        fr = planes[slot, :, pl.ds((2 * color) * plane, plane)]
        fi = planes[slot, :, pl.ds((2 * color + 1) * plane, plane)]
        coeff = jnp.concatenate([rows(which, 0), rows(which, 1)], 0)
        n = coeff.shape[0] // 2
        yr = split_dot(coeff, fr)
        yi = split_dot(coeff, fi)
        return yr[:n] - yi[n:], yi[:n] + yr[n:]

    def own_rows(which, part):
        return pts[which, part, pl.ds(first_row, rows0), :]

    def all_rows(which, part):
        return pts[which, part]

    for color in range(3):
        re, im = turned(0, own_rows, color)
        u_ref[slot, 2 * color] = re
        u_ref[slot, 2 * color + 1] = im
        if not pair:
            continue
        at = pl.ds(pl.multiple_of((slot - 1) * plane, plane), plane)
        parts, each = v_ref.shape[1:3]
        re, im = turned(1, all_rows, color)
        for d in range(parts):
            low = slice(2 * d * each, (2 * d + 1) * each)
            high = slice((2 * d + 1) * each, (2 * d + 2) * each)
            vr = jnp.where(parity == 0, re[low], re[high])
            vi = jnp.where(parity == 0, im[low], im[high])
            v_ref[3 * color, d, :, at] = vr
            v_ref[3 * color + 1, d, :, at] = vi
            v_ref[3 * color + 2, d, :, at] = vr + vi
        re, im = turned(2, all_rows, color)
        re = re.astype(BF16)
        im = im.astype(BF16)
        rhs_ref[2 * color, pl.ds(0, count), at] = re
        rhs_ref[2 * color, pl.ds(count, count), at] = im
        rhs_ref[2 * color + 1, pl.ds(0, count), at] = -im
        rhs_ref[2 * color + 1, pl.ds(count, count), at] = re


def displace(weights, phases, links, below, u_ref, p_ref, plane):
    tile = 8
    xcoord = lax.broadcasted_iota(jnp.int32, (tile, plane), 1) % LX

    def one(step, carry):
        rows = pl.ds(pl.multiple_of(step * tile, tile), tile)

        def load(index):
            return [(u_ref[index, 2 * c, rows, :], u_ref[index, 2 * c + 1, rows, :]) for c in range(3)]

        for own in range(2):
            def own_link(direction, row, col, own=own):
                return tuple(links[own, direction, row, col, c] for c in range(2))

            def below_link(row, col, own=own):
                if own == 1:
                    return own_link(2, row, col, 0)
                return tuple(below[row, col, c] for c in range(2))

            here = load(own + 1)
            total = [[None, None] for _ in range(3)]
            for direction in range(3):
                if direction == 0:
                    ahead = [(shift_x(r, True, xcoord), shift_x(i, True, xcoord)) for r, i in here]
                    back = adjoint_times(own_link, (0,), here)
                    back = [(shift_x(r, False, xcoord), shift_x(i, False, xcoord)) for r, i in back]
                elif direction == 1:
                    ahead = [(shift_y(r, True), shift_y(i, True)) for r, i in here]
                    back = adjoint_times(own_link, (1,), here)
                    back = [(shift_y(r, False), shift_y(i, False)) for r, i in back]
                else:
                    ahead = load(own + 2)
                    back = adjoint_times(below_link, (), load(own))
                front = link_times(own_link, (direction,), ahead)
                factor = weights[direction].astype(F32)
                for k in range(3):
                    for c in range(2):
                        term = factor * (front[k][c] - back[k][c])
                        total[k][c] = term if total[k][c] is None else total[k][c] + term
            cosine, sine = phases[own]
            at = pl.ds(own * plane, plane)
            for k in range(3):
                re = cosine * total[k][0] + sine * total[k][1]
                im = cosine * total[k][1] - sine * total[k][0]
                p_ref[3 * k, rows, at] = re
                p_ref[3 * k + 1, rows, at] = im
                p_ref[3 * k + 2, rows, at] = re + im
        return carry

    lax.fori_loop(0, p_ref.shape[1] // tile, one, 0)


def cross_tile(m_ref, p_ref, v_ref, part, lanes, lane, r):
    rows = p_ref.shape[1]
    at = pl.ds(pl.multiple_of(lanes + lane, 128), 128)
    p = [p_ref[c, pl.ds(r, 16), at] for c in range(9)]
    for b in range(v_ref.shape[2]):
        v = [v_ref[c, part, pl.ds(b, 1), at] for c in range(9)]
        to = pl.ds(pl.multiple_of(b * rows + r, 16), 16)
        for j in range(3):
            k, i = (j + 1) % 3, (j + 2) % 3
            t = [p[3 * k + s] * v[3 * i + s] - p[3 * i + s] * v[3 * k + s] for s in range(3)]
            re = t[0] - t[1]
            im = t[2] - (t[0] + t[1])
            m_ref[2 * j, to, pl.ds(lane, 128)] = re.astype(BF16)
            m_ref[2 * j + 1, to, pl.ds(lane, 128)] = im.astype(BF16)


def mixed(next_ref, now_ref, p_ref, v_ref, rhs_ref, acc, part, lanes, now_lanes, now_first):
    width = next_ref.shape[2]
    rows = p_ref.shape[1]
    at = pl.ds(pl.multiple_of(now_lanes, 128), width)

    def body(t, carry):
        total = None
        for j in range(2):
            term = lax.dot_general(
                now_ref[2 * t + j],
                rhs_ref[2 * t + j, :, at],
                (((1,), (1,)), ((), ())),
                preferred_element_type=F32,
            )
            total = term if total is None else total + term
        r = pl.multiple_of(t * 16, 16)
        for lane in range(0, width, 128):
            cross_tile(next_ref, p_ref, v_ref, part, lanes, lane, r)
        keep = jnp.where(jnp.logical_and(now_first, t == 0), 0.0, 1.0)
        acc[...] = acc[...] * keep + total
        return carry

    lax.fori_loop(0, 3, body, 0)


def block_kernel(names, weights, momentum, spins, own_ref, links_ref, peram_hbm, o_ref, peram, pts,
                 planes, links, below, u_ref, p_ref, v_ref, rhs_ref, acc, m0, m1, stage, arrived, psend, precv, ssend,
                 srecv, lsend, lrecv, bsend, brecv, rsend, rrecv, jsend, jrecv, xsend, xrecv, csem):
    gz, ea, ndev = names
    me = lax.axis_index(gz)
    core = lax.axis_index(ea)
    odd = me % 2
    half = ndev // 2
    local, width6 = own_ref.shape
    plane = width6 // 6

    def at_gz(index):
        return {gz: index}

    sibling = {ea: 1 - core}
    mate = me + 1 - 2 * odd
    jump = lax.rem(me + ndev - 2 + 4 * odd, ndev)
    fetch = pltpu.make_async_copy(peram_hbm, peram, csem)
    fetch.start()

    def same_parity(t):
        return lax.rem(me + 2 * t, ndev)

    barrier = pltpu.get_barrier_semaphore()
    friends = [sibling, at_gz(mate)] + [at_gz(same_parity(t)) for t in range(1, half)]
    for friend in friends:
        pl.semaphore_signal(barrier, inc=1, device_id=friend, device_id_type=pl.DeviceIdType.MESH)
    pl.semaphore_wait(barrier, len(friends))

    piece = 16
    pieces = local // piece
    my_first = core * local
    her_first = (1 - core) * local
    my_slot = 1 + odd
    mate_slot = 2 - odd
    jump_slot = 3 - 3 * odd
    far_slot = 3 * odd

    def span(first, n=None):
        if n is None:
            return pl.ds(pl.multiple_of(first, 16), local)
        return pl.ds(pl.multiple_of(first + n * piece, 16), piece)

    def remote(src, dst, send, recv, device):
        return pltpu.make_async_remote_copy(
            src_ref=src, dst_ref=dst, send_sem=send, recv_sem=recv, device_id=device,
            device_id_type=pl.DeviceIdType.MESH,
        )

    def to_jump(n):
        return remote(
            own_ref.at[pl.ds(n * piece, piece)], planes.at[jump_slot, span(my_first, n)],
            jsend.at[n], jrecv.at[n], at_gz(jump),
        )

    def z_links():
        return remote(links_ref.at[2], below, bsend, brecv, at_gz(jump))

    def z_relay():
        return remote(below, below, bsend, brecv, at_gz(mate))

    def relay(slot, n):
        block = planes.at[slot, span(my_first, n)]
        return remote(block, block, xsend.at[n], xrecv.at[n], at_gz(mate))

    def share(slot, first):
        block = planes.at[slot, span(first)]
        return remote(block, block, ssend.at[slot], srecv.at[slot], sibling)

    for n in range(pieces):
        to_jump(n).start()

    @pl.when(odd == 1)
    def _():
        z_links().start()

    share_own = remote(
        own_ref, planes.at[my_slot, span(my_first)], ssend.at[my_slot], srecv.at[my_slot], sibling
    )
    share_own.start()
    to_mate = remote(own_ref, planes.at[my_slot, span(my_first)], psend, precv, at_gz(mate))
    to_mate.start()
    link_mate = remote(links_ref, links.at[odd], lsend, lrecv.at[odd], at_gz(mate))
    link_mate.start()
    planes[my_slot, span(my_first), :] = own_ref[...]
    links[odd] = links_ref[...]
    fetch.wait()
    for q in range(3):
        for c in range(2):
            pts[q, c] = peram[spins[q, 0], spins[q, 1], c].T

    def fill(slot, pair):
        fill_fields(slot, pair, planes, pts, pl.multiple_of(my_first, 8), odd, u_ref, v_ref,
                    rhs_ref, plane)

    share(my_slot, her_first).wait_recv()
    fill(my_slot, True)
    to_jump(0).wait_recv()
    relay(jump_slot, 0).start()
    remote(own_ref, planes.at[mate_slot, span(my_first)], psend, precv, at_gz(mate)).wait_recv()
    share(mate_slot, my_first).start()
    for n in range(1, pieces - 1):
        to_jump(n).wait_recv()
        relay(jump_slot, n).start()
    share(mate_slot, her_first).wait_recv()
    fill(mate_slot, True)
    for n in range(max(pieces - 1, 1), pieces):
        to_jump(n).wait_recv()
        relay(jump_slot, n).start()
    share(jump_slot, my_first).start()

    @pl.when(odd == 1)
    def _():
        z_links().wait_send()
        z_links().wait_recv()
        z_relay().start()

    @pl.when(odd == 0)
    def _():
        z_relay().wait_recv()

    share(jump_slot, her_first).wait_recv()
    fill(jump_slot, False)
    for n in range(pieces):
        relay(far_slot, n).wait_recv()
    share(far_slot, my_first).start()
    share(far_slot, her_first).wait_recv()
    fill(far_slot, False)
    remote(links_ref, links.at[1 - odd], lsend, lrecv.at[1 - odd], at_gz(mate)).wait_recv()

    sites = lax.broadcasted_iota(jnp.int32, (1, plane), 1)
    two_pi = 2.0 * math.pi
    scale = 1.0 / math.sqrt(plane * ndev)
    inplane = (momentum[0] * (sites % LX)).astype(F32) / LX + (
        momentum[1] * (sites // LX)
    ).astype(F32) / LY
    phases = []
    for own in range(2):
        height = jnp.full((1, plane), momentum[2] * (me - odd + own), jnp.int32).astype(F32)
        angle = two_pi * inplane + two_pi * height / ndev
        phases.append((jnp.cos(angle) * scale, jnp.sin(angle) * scale))
    displace(weights, phases, links, below, u_ref, p_ref, plane)

    width = m0.shape[2]
    chunks = p_ref.shape[2] // width
    total = half * chunks
    zplace = me // 2

    def place(n):
        return lax.rem(zplace + 1 + n // chunks, half), (n % chunks) * width

    part, lanes = place(0)

    def begin(t, carry):
        for lane in range(0, width, 128):
            cross_tile(m0, p_ref, v_ref, part, lanes, lane, pl.multiple_of(t * 16, 16))
        return carry

    lax.fori_loop(0, 3, begin, 0)
    rows = p_ref.shape[1]
    wide = acc.shape[1] // 2

    def lay_out(put):
        for b in range(v_ref.shape[2]):
            for c in range(2):
                put(c, pl.ds(b * wide, wide), acc[pl.ds(b * rows, rows), pl.ds(c * wide, wide)])

    def send(t):
        return remote(stage.at[t], arrived.at[t], rsend.at[t], rrecv.at[t], at_gz(same_parity(t + 1)))

    def stretch(n, carry):
        for sub, (now, after) in enumerate(((m0, m1), (m1, m0))):
            step = 2 * n + sub
            now_part, now_lanes = place(step)
            part, lanes = place(jnp.minimum(step + 1, total - 1))
            mixed(after, now, p_ref, v_ref, rhs_ref, acc, part, lanes, now_lanes, step % chunks == 0)
        return carry

    def one_part(d, carry):
        lax.fori_loop(d * (chunks // 2), (d + 1) * (chunks // 2), stretch, 0)

        @pl.when(d < half - 1)
        def _():
            def put(c, at, block):
                stage[d, c, :, at] = block.astype(BF16)

            lay_out(put)
            send(d).start()

        return carry

    lax.fori_loop(0, half, one_part, 0)

    def put_own(c, at, block):
        o_ref[c, :, at] = block

    lay_out(put_own)
    for t in range(half - 1):
        send(t).wait_recv()
        o_ref[...] += arrived[t].astype(F32)
    for t in range(half - 1):
        send(t).wait_send()
    to_mate.wait_send()
    link_mate.wait_send()
    for n in range(pieces):
        to_jump(n).wait_send()
        relay(jump_slot, n).wait_send()
    for slot in range(4):
        share(slot, my_first).wait_send()

    @pl.when(odd == 1)
    def _():
        z_relay().wait_send()


def shards(eigvec, links, momentum, weights, spins, peram):
    local = eigvec.shape[0]
    plane = eigvec.shape[4]
    ndev = lax.axis_size("gz")
    count = peram.shape[-1]
    each = count // ndev
    half = ndev // 2
    own = eigvec.reshape(local, 6 * plane)
    vmem = pl.BlockSpec(memory_space=pltpu.VMEM)
    smem = pl.BlockSpec(memory_space=pltpu.SMEM)
    total = 2 * plane
    width = 256
    rows = each * local
    dma = pltpu.SemaphoreType.DMA
    out = pl.pallas_call(
        functools.partial(block_kernel, ("gz", "ea", ndev)),
        out_shape=jax.ShapeDtypeStruct((2, local, each * count), F32),
        in_specs=[smem, smem, smem, vmem, vmem, pl.BlockSpec(memory_space=pl.ANY)],
        out_specs=vmem,
        scratch_shapes=[
            pltpu.VMEM(peram.shape, F32),
            pltpu.VMEM((3, 2, count, count), F32),
            pltpu.VMEM((4, 2 * local, 6 * plane), BF16),
            pltpu.VMEM((2,) + links.shape, F32),
            pltpu.VMEM(links.shape[1:], F32),
            pltpu.VMEM((4, 6, local, plane), F32),
            pltpu.VMEM((9, local, total), F32),
            pltpu.VMEM((9, half, each, total), F32),
            pltpu.VMEM((6, 2 * count, total), BF16),
            pltpu.VMEM((rows, 2 * count), F32),
            pltpu.VMEM((6, rows, width), BF16),
            pltpu.VMEM((6, rows, width), BF16),
            pltpu.VMEM((half - 1, 2, local, each * count), BF16),
            pltpu.VMEM((half - 1, 2, local, each * count), BF16),
            dma,
            dma,
            dma((4,)),
            dma((4,)),
            dma,
            dma((2,)),
            dma,
            dma,
            dma((half - 1,)),
            dma((half - 1,)),
            dma((local // 16,)),
            dma((local // 16,)),
            dma((local // 16,)),
            dma((local // 16,)),
            dma,
        ],
        compiler_params=pltpu.CompilerParams(
            vmem_limit_bytes=62 * 1024 * 1024, collective_id=0, has_side_effects=True
        ),
        name="block",
    )(weights, momentum, spins, own, links, peram)
    return out


def solution(mesh):
    ndev = mesh.shape["gz"]
    in_specs = (
        P("ea", None, None, ("groups", "gz"), None),
        P(None, None, None, None, ("groups", "gz"), None),
        P("groups"),
        P("groups"),
        P("groups", None),
        P("groups", None, None, None, None),
    )
    out_specs = P("groups", "ea", "gz")

    def body(eigvec, links, momentum, weights, spins, peram):
        whole_rows = peram.shape[-1] % (2 * ndev) == 0 and ndev % 2 == 0 and ndev > 2
        whole_rows = whole_rows and eigvec.shape[0] % 16 == 0 and eigvec.shape[3] == 1
        run = shards if whole_rows else plain_shards
        return run(eigvec, links, momentum, weights, spins, peram)

    return jax.shard_map(body, mesh=mesh, in_specs=in_specs, out_specs=out_specs, check_vma=False)
```

```python
import functools
import math

import jax
import jax.numpy as jnp
from jax import lax
from jax.experimental import pallas as pl
from jax.experimental.pallas import tpu as pltpu
from jax.sharding import PartitionSpec as P

LX = 32
LY = 16
F32 = jnp.float32
BF16 = jnp.bfloat16
NT = (((1,), (0,)), ((), ()))


def from_behind(array, axis, by):
    count = lax.axis_size(axis)
    return lax.ppermute(array, axis, [(i, (i + by) % count) for i in range(count)])


def plain_link(link, lattice_field):
    result_real = 0.0
    result_imaginary = 0.0
    for column_slot in range(3):
        gauge_link_real = link[None, :, column_slot, 0]
        gauge_link_imaginary = link[None, :, column_slot, 1]
        vector_real = lattice_field[:, None, column_slot, 0]
        vector_imaginary = lattice_field[:, None, column_slot, 1]
        result_real = (
            result_real + gauge_link_real * vector_real - gauge_link_imaginary * vector_imaginary
        )
        result_imaginary = (
            result_imaginary
            + gauge_link_real * vector_imaginary
            + gauge_link_imaginary * vector_real
        )
    return jnp.stack([result_real, result_imaginary], 2)


def adjoint_apply(link, lattice_field):
    result_real = 0.0
    result_imaginary = 0.0
    for column_slot in range(3):
        gauge_link_real = link[None, column_slot, :, 0]
        gauge_link_imaginary = link[None, column_slot, :, 1]
        vector_real = lattice_field[:, None, column_slot, 0]
        vector_imaginary = lattice_field[:, None, column_slot, 1]
        result_real = (
            result_real + gauge_link_real * vector_real + gauge_link_imaginary * vector_imaginary
        )
        result_imaginary = (
            result_imaginary
            + gauge_link_real * vector_imaginary
            - gauge_link_imaginary * vector_real
        )
    return jnp.stack([result_real, result_imaginary], 2)


def cross_parts(left_vec, right_vec):
    reals = []
    imags = []
    for first, second in ((1, 2), (2, 0), (0, 1)):
        ar = left_vec[:, :, first, 0]
        ai = left_vec[:, :, first, 1]
        br = left_vec[:, :, second, 0]
        bi = left_vec[:, :, second, 1]
        cr = right_vec[:, :, first, 0]
        ci = right_vec[:, :, first, 1]
        dr = right_vec[:, :, second, 0]
        di = right_vec[:, :, second, 1]
        reals.append(ar * dr - ai * di - (br * cr - bi * ci))
        imags.append(ar * di + ai * dr - (br * ci + bi * cr))
    return jnp.stack([jnp.stack(reals), jnp.stack(imags)])


def mode_product(lattice_field, block, form):
    high = lax.Precision.HIGHEST
    real_part = jnp.einsum(form, lattice_field[0], block[0], precision=high) - jnp.einsum(
        form, lattice_field[1], block[1], precision=high
    )
    imag_part = jnp.einsum(form, lattice_field[0], block[1], precision=high) + jnp.einsum(
        form, lattice_field[1], block[0], precision=high
    )
    return jnp.stack([real_part, imag_part])


def roll_plane(lattice_field, direction, amount):
    grid = lattice_field.reshape(lattice_field.shape[:-1] + (LY, LX))
    axis_here = grid.ndim - 1 if direction == 0 else grid.ndim - 2
    return jnp.roll(grid, amount, axis_here).reshape(lattice_field.shape)


def elemental_part(phased, vectors):
    count = vectors.shape[0]
    size_a = phased.shape[0]
    nsites = vectors.shape[3]
    real_part = phased[:, :, 0]
    imag_part = phased[:, :, 1]
    upper_rows = jnp.stack([real_part, -imag_part], 1)
    lower_rows = jnp.stack([imag_part, real_part], 1)
    left = jnp.stack([upper_rows, lower_rows], 0).reshape(2 * size_a, 2, 3, nsites)
    width = min(8, count)
    others = vectors.astype(jnp.float32)[None]

    def one_block(rows):
        wmat = cross_parts(rows.astype(jnp.float32)[:, None], others).astype(jnp.bfloat16)
        return jnp.einsum("xrks,rkbcs->xbc", left, wmat, preferred_element_type=jnp.float32)

    result = lax.map(one_block, vectors.reshape(count // width, width, 3, 2, nsites))
    return result.transpose(1, 0, 2, 3).reshape(2, size_a, count * count)


def plain_shards(eigvec, links, momentum, weights, spins, peram):
    local_vecs = eigvec.shape[0]
    planes = eigvec.shape[3]
    plane = eigvec.shape[4]
    depth = planes * lax.axis_size("gz")
    vecf = eigvec.astype(jnp.float32)
    disp = jnp.zeros(vecf.shape, jnp.float32)
    for direction in range(3):
        link = links[direction]
        back = adjoint_apply(link, vecf).astype(jnp.bfloat16)
        if direction == 2:
            upper = from_behind(eigvec, "gz", -1)
            ahead = jnp.concatenate([eigvec[:, :, :, 1:], upper], axis=3).astype(jnp.float32)
            lower = from_behind(back, "gz", 1)
            behind = jnp.concatenate([lower, back[:, :, :, :-1]], axis=3)
        else:
            ahead = roll_plane(vecf, direction, -1)
            behind = roll_plane(back, direction, 1)
        behind = lax.optimization_barrier(behind).astype(jnp.float32)
        factor = weights[direction].astype(jnp.float32)
        disp = disp + factor * (plain_link(link, ahead) - behind)
    sites = jnp.arange(plane, dtype=jnp.int32)
    xcoord = sites % LX
    ycoord = sites // LX
    zcoord = lax.axis_index("gz") * planes + jnp.arange(planes, dtype=jnp.int32)
    two_pi = 2.0 * math.pi
    inplane = (momentum[0] * xcoord).astype(jnp.float32) / LX + (momentum[1] * ycoord).astype(
        jnp.float32
    ) / LY
    angle = (
        two_pi * inplane[None, :]
        + two_pi * (momentum[2] * zcoord).astype(jnp.float32)[:, None] / depth
    )
    cosine = jnp.cos(angle)
    sine = jnp.sin(angle)
    phased_re = cosine * disp[:, :, 0] + sine * disp[:, :, 1]
    phased_im = cosine * disp[:, :, 1] - sine * disp[:, :, 0]
    phased = jnp.stack([phased_re, phased_im], 2).astype(jnp.bfloat16)
    nsites = planes * plane
    phased = phased.reshape(local_vecs, 3, 2, nsites)
    flat_vecs = eigvec.reshape(local_vecs, 3, 2, nsites)
    scale = 1.0 / math.sqrt(LX * LY * depth)
    blocks = [peram[spins[q, 0], spins[q, 1]] for q in range(3)]
    every = lax.all_gather(flat_vecs, "ea", axis=0, tiled=True)
    count = every.shape[0]
    partial_value = elemental_part(phased, every) * scale
    partial_value = partial_value.reshape(2, local_vecs, count, count)
    partial_value = mode_product(partial_value, blocks[2], "abc,cf->abf")
    partial_value = mode_product(partial_value, blocks[1], "abc,be->aec")
    partial_value = partial_value.reshape(2, local_vecs, count * count)
    summed = lax.psum_scatter(partial_value, "gz", scatter_dimension=2, tiled=True)
    rows = lax.dynamic_slice_in_dim(blocks[0], lax.axis_index("ea") * local_vecs, local_vecs, 1)
    term = mode_product(summed, rows, "ak,ad->dk")
    return lax.psum_scatter(term, "ea", scatter_dimension=1, tiled=True)


def split_dot(coeff, field):
    high = coeff.astype(BF16)
    low = (coeff - high.astype(F32)).astype(BF16)
    return lax.dot_general(high, field, NT, preferred_element_type=F32) + lax.dot_general(
        low, field, NT, preferred_element_type=F32
    )


def shift_x(field, ahead, xcoord):
    size = field.shape[-1]
    if ahead:
        return jnp.where(
            xcoord == LX - 1, pltpu.roll(field, LX - 1, 1), pltpu.roll(field, size - 1, 1)
        )
    return jnp.where(xcoord == 0, pltpu.roll(field, size - LX + 1, 1), pltpu.roll(field, 1, 1))


def shift_y(field, ahead):
    size = field.shape[-1]
    return pltpu.roll(field, size - LX if ahead else LX, 1)


def link_times(links, index, field):
    out = []
    for row in range(3):
        re = im = None
        for col in range(3):
            ur, ui = links(*index, row, col)
            vr, vi = field[col]
            a = ur * vr - ui * vi
            b = ur * vi + ui * vr
            re = a if re is None else re + a
            im = b if im is None else im + b
        out.append((re, im))
    return out


def adjoint_times(links, index, field):
    out = []
    for row in range(3):
        re = im = None
        for col in range(3):
            ur, ui = links(*index, col, row)
            vr, vi = field[col]
            a = ur * vr + ui * vi
            b = ur * vi - ui * vr
            re = a if re is None else re + a
            im = b if im is None else im + b
        out.append((re, im))
    return out


def fill_fields(slot, pair, planes, pts, first_row, parity, u_ref, v_ref, rhs_ref, plane):
    rows0 = u_ref.shape[2]
    count = pts.shape[2]

    def turned(which, rows, color):
        fr = planes[slot, :, pl.ds((2 * color) * plane, plane)]
        fi = planes[slot, :, pl.ds((2 * color + 1) * plane, plane)]
        coeff = jnp.concatenate([rows(which, 0), rows(which, 1)], 0)
        n = coeff.shape[0] // 2
        yr = split_dot(coeff, fr)
        yi = split_dot(coeff, fi)
        return yr[:n] - yi[n:], yi[:n] + yr[n:]

    def own_rows(which, part):
        return pts[which, part, pl.ds(first_row, rows0), :]

    def all_rows(which, part):
        return pts[which, part]

    for color in range(3):
        re, im = turned(0, own_rows, color)
        u_ref[slot, 2 * color] = re
        u_ref[slot, 2 * color + 1] = im
        if not pair:
            continue
        at = pl.ds(pl.multiple_of((slot - 1) * plane, plane), plane)
        parts, each = v_ref.shape[1:3]
        re, im = turned(1, all_rows, color)
        for d in range(parts):
            low = slice(2 * d * each, (2 * d + 1) * each)
            high = slice((2 * d + 1) * each, (2 * d + 2) * each)
            vr = jnp.where(parity == 0, re[low], re[high])
            vi = jnp.where(parity == 0, im[low], im[high])
            v_ref[3 * color, d, :, at] = vr
            v_ref[3 * color + 1, d, :, at] = vi
            v_ref[3 * color + 2, d, :, at] = vr + vi
        re, im = turned(2, all_rows, color)
        re = re.astype(BF16)
        im = im.astype(BF16)
        rhs_ref[2 * color, pl.ds(0, count), at] = re
        rhs_ref[2 * color, pl.ds(count, count), at] = im
        rhs_ref[2 * color + 1, pl.ds(0, count), at] = -im
        rhs_ref[2 * color + 1, pl.ds(count, count), at] = re


def displace(weights, phases, links, below, u_ref, p_ref, plane):
    tile = 8
    xcoord = lax.broadcasted_iota(jnp.int32, (tile, plane), 1) % LX

    def one(step, carry):
        rows = pl.ds(pl.multiple_of(step * tile, tile), tile)

        def load(index):
            return [(u_ref[index, 2 * c, rows, :], u_ref[index, 2 * c + 1, rows, :]) for c in range(3)]

        for own in range(2):
            def own_link(direction, row, col, own=own):
                return tuple(links[own, direction, row, col, c] for c in range(2))

            def below_link(row, col, own=own):
                if own == 1:
                    return own_link(2, row, col, 0)
                return tuple(below[row, col, c] for c in range(2))

            here = load(own + 1)
            total = [[None, None] for _ in range(3)]
            for direction in range(3):
                if direction == 0:
                    ahead = [(shift_x(r, True, xcoord), shift_x(i, True, xcoord)) for r, i in here]
                    back = adjoint_times(own_link, (0,), here)
                    back = [(shift_x(r, False, xcoord), shift_x(i, False, xcoord)) for r, i in back]
                elif direction == 1:
                    ahead = [(shift_y(r, True), shift_y(i, True)) for r, i in here]
                    back = adjoint_times(own_link, (1,), here)
                    back = [(shift_y(r, False), shift_y(i, False)) for r, i in back]
                else:
                    ahead = load(own + 2)
                    back = adjoint_times(below_link, (), load(own))
                front = link_times(own_link, (direction,), ahead)
                factor = weights[direction].astype(F32)
                for k in range(3):
                    for c in range(2):
                        term = factor * (front[k][c] - back[k][c])
                        total[k][c] = term if total[k][c] is None else total[k][c] + term
            cosine, sine = phases[own]
            at = pl.ds(own * plane, plane)
            for k in range(3):
                re = cosine * total[k][0] + sine * total[k][1]
                im = cosine * total[k][1] - sine * total[k][0]
                p_ref[3 * k, rows, at] = re
                p_ref[3 * k + 1, rows, at] = im
                p_ref[3 * k + 2, rows, at] = re + im
        return carry

    lax.fori_loop(0, p_ref.shape[1] // tile, one, 0)


def cross_tile(m_ref, p_ref, v_ref, part, lanes, lane, r):
    rows = p_ref.shape[1]
    at = pl.ds(pl.multiple_of(lanes + lane, 128), 128)
    p = [p_ref[c, pl.ds(r, 16), at] for c in range(9)]
    for b in range(v_ref.shape[2]):
        v = [v_ref[c, part, pl.ds(b, 1), at] for c in range(9)]
        to = pl.ds(pl.multiple_of(b * rows + r, 16), 16)
        for j in range(3):
            k, i = (j + 1) % 3, (j + 2) % 3
            t = [p[3 * k + s] * v[3 * i + s] - p[3 * i + s] * v[3 * k + s] for s in range(3)]
            re = t[0] - t[1]
            im = t[2] - (t[0] + t[1])
            m_ref[2 * j, to, pl.ds(lane, 128)] = re.astype(BF16)
            m_ref[2 * j + 1, to, pl.ds(lane, 128)] = im.astype(BF16)


def mixed(next_ref, now_ref, p_ref, v_ref, rhs_ref, acc, part, lanes, now_lanes):
    width = next_ref.shape[2]
    rows = p_ref.shape[1]
    at = pl.ds(pl.multiple_of(now_lanes, 128), width)

    def body(t, carry):
        total = None
        for j in range(2):
            term = lax.dot_general(
                now_ref[2 * t + j],
                rhs_ref[2 * t + j, :, at],
                (((1,), (1,)), ((), ())),
                preferred_element_type=F32,
            )
            total = term if total is None else total + term
        r = pl.multiple_of(t * 16, 16)
        for lane in range(0, width, 128):
            cross_tile(next_ref, p_ref, v_ref, part, lanes, lane, r)
        acc[...] += total
        return carry

    lax.fori_loop(0, 3, body, 0)


def block_kernel(names, weights, momentum, spins, own_ref, links_ref, peram_hbm, o_ref, peram, pts,
                 planes, links, below, u_ref, p_ref, v_ref, rhs_ref, acc, m0, m1, stage, arrived, psend, precv, ssend,
                 srecv, lsend, lrecv, bsend, brecv, rsend, rrecv, jsend, jrecv, xsend, xrecv, csem):
    gz, ea, ndev = names
    me = lax.axis_index(gz)
    core = lax.axis_index(ea)
    odd = me % 2
    half = ndev // 2
    local, width6 = own_ref.shape
    plane = width6 // 6

    def at_gz(index):
        return {gz: index}

    sibling = {ea: 1 - core}
    mate = me + 1 - 2 * odd
    jump = lax.rem(me + ndev - 2 + 4 * odd, ndev)
    hop = lax.rem(me + ndev + 2 - 4 * odd, ndev)
    fetch = pltpu.make_async_copy(peram_hbm, peram, csem)
    fetch.start()

    def same_parity(t):
        return lax.rem(me + 2 * t, ndev)

    barrier = pltpu.get_barrier_semaphore()
    friends = [sibling, at_gz(mate)] + [at_gz(same_parity(t)) for t in range(1, half)]
    for friend in friends:
        pl.semaphore_signal(barrier, inc=1, device_id=friend, device_id_type=pl.DeviceIdType.MESH)
    pl.semaphore_wait(barrier, len(friends))

    piece = 16
    pieces = local // piece
    my_first = core * local
    her_first = (1 - core) * local
    my_slot = 1 + odd
    mate_slot = 2 - odd
    jump_slot = 3 - 3 * odd
    far_slot = 3 * odd

    def span(first, n=None):
        if n is None:
            return pl.ds(pl.multiple_of(first, 16), local)
        return pl.ds(pl.multiple_of(first + n * piece, 16), piece)

    def remote(src, dst, send, recv, device):
        return pltpu.make_async_remote_copy(
            src_ref=src, dst_ref=dst, send_sem=send, recv_sem=recv, device_id=device,
            device_id_type=pl.DeviceIdType.MESH,
        )

    def to_jump(n):
        return remote(
            own_ref.at[pl.ds(n * piece, piece)], planes.at[jump_slot, span(my_first, n)],
            jsend.at[n], jrecv.at[n], at_gz(jump),
        )

    def z_links():
        return remote(links_ref.at[2], below, bsend, brecv, at_gz(jump))

    def z_relay():
        return remote(links.at[1 - odd, 2], below, bsend, brecv, at_gz(hop))

    def relay(n):
        return remote(
            planes.at[mate_slot, span(my_first, n)], planes.at[far_slot, span(my_first, n)],
            xsend.at[n], xrecv.at[n], at_gz(hop),
        )

    def to_mate(n):
        return remote(
            own_ref.at[pl.ds(n * piece, piece)], planes.at[my_slot, span(my_first, n)],
            psend.at[n], precv.at[n], at_gz(mate),
        )

    def share(slot, first):
        block = planes.at[slot, span(first)]
        return remote(block, block, ssend.at[slot], srecv.at[slot], sibling)

    for n in range(pieces):
        to_mate(n).start()
        to_jump(n).start()

    @pl.when(odd == 1)
    def _():
        z_links().start()

    share_own = remote(
        own_ref, planes.at[my_slot, span(my_first)], ssend.at[my_slot], srecv.at[my_slot], sibling
    )
    share_own.start()
    link_mate = remote(links_ref, links.at[odd], lsend, lrecv.at[odd], at_gz(mate))
    link_mate.start()
    planes[my_slot, span(my_first), :] = own_ref[...]
    links[odd] = links_ref[...]
    fetch.wait()
    for q in range(3):
        for c in range(2):
            pts[q, c] = peram[spins[0, q], spins[1, q], c].T

    def fill(slot, pair):
        fill_fields(slot, pair, planes, pts, pl.multiple_of(my_first, 8), odd, u_ref, v_ref,
                    rhs_ref, plane)

    share(my_slot, her_first).wait_recv()
    fill(my_slot, True)
    for n in range(pieces):
        to_mate(n).wait_recv()
        relay(n).start()
    share(mate_slot, my_first).start()
    share(mate_slot, her_first).wait_recv()
    fill(mate_slot, True)
    for n in range(pieces):
        to_jump(n).wait_recv()
    share(jump_slot, my_first).start()
    remote(links_ref, links.at[1 - odd], lsend, lrecv.at[1 - odd], at_gz(mate)).wait_recv()

    @pl.when(odd == 0)
    def _():
        z_relay().start()

    share(jump_slot, her_first).wait_recv()
    fill(jump_slot, False)
    for n in range(pieces):
        relay(n).wait_recv()
    share(far_slot, my_first).start()
    share(far_slot, her_first).wait_recv()
    fill(far_slot, False)
    z_relay().wait_recv()

    sites = lax.broadcasted_iota(jnp.int32, (1, plane), 1)
    two_pi = 2.0 * math.pi
    scale = 1.0 / math.sqrt(plane * ndev)
    inplane = (momentum[0] * (sites % LX)).astype(F32) / LX + (
        momentum[1] * (sites // LX)
    ).astype(F32) / LY
    phases = []
    for own in range(2):
        height = jnp.full((1, plane), momentum[2] * (me - odd + own), jnp.int32).astype(F32)
        angle = two_pi * inplane + two_pi * height / ndev
        phases.append((jnp.cos(angle) * scale, jnp.sin(angle) * scale))
    displace(weights, phases, links, below, u_ref, p_ref, plane)

    width = m0.shape[2]
    chunks = p_ref.shape[2] // width
    total = half * chunks
    zplace = me // 2

    def place(n):
        return lax.rem(zplace + 1 + n // chunks, half), (n % chunks) * width

    part, lanes = place(0)

    def begin(t, carry):
        for lane in range(0, width, 128):
            cross_tile(m0, p_ref, v_ref, part, lanes, lane, pl.multiple_of(t * 16, 16))
        return carry

    lax.fori_loop(0, 3, begin, 0)
    rows = p_ref.shape[1]
    wide = acc.shape[1] // 2

    def lay_out(put):
        for b in range(v_ref.shape[2]):
            for c in range(2):
                put(c, pl.ds(b * wide, wide), acc[pl.ds(b * rows, rows), pl.ds(c * wide, wide)])

    def send(t):
        return remote(stage.at[t], arrived.at[t], rsend.at[t], rrecv.at[t], at_gz(same_parity(t + 1)))

    def stretch(n, carry):
        for sub, (now, after) in enumerate(((m0, m1), (m1, m0))):
            step = 2 * n + sub
            now_part, now_lanes = place(step)
            part, lanes = place(jnp.minimum(step + 1, total - 1))
            mixed(after, now, p_ref, v_ref, rhs_ref, acc, part, lanes, now_lanes)
        return carry

    def one_part(d, carry):
        acc[...] = jnp.zeros_like(acc)
        lax.fori_loop(d * (chunks // 2), (d + 1) * (chunks // 2), stretch, 0)

        @pl.when(d < half - 1)
        def _():
            def put(c, at, block):
                stage[d, c, :, at] = block.astype(BF16)

            lay_out(put)
            send(d).start()

        return carry

    lax.fori_loop(0, half, one_part, 0)

    def put_own(c, at, block):
        o_ref[c, :, at] = block

    lay_out(put_own)
    for t in range(half - 1):
        send(t).wait_recv()
        o_ref[...] += arrived[t].astype(F32)
    for t in range(half - 1):
        send(t).wait_send()
    link_mate.wait_send()
    for n in range(pieces):
        to_mate(n).wait_send()
        to_jump(n).wait_send()
        relay(n).wait_send()
    for slot in range(4):
        share(slot, my_first).wait_send()
    z_relay().wait_send()


def shards(eigvec, links, momentum, weights, spins, peram):
    local = eigvec.shape[0]
    plane = eigvec.shape[4]
    ndev = lax.axis_size("gz")
    count = peram.shape[-1]
    each = count // ndev
    half = ndev // 2
    own = eigvec.reshape(local, 6 * plane)
    vmem = pl.BlockSpec(memory_space=pltpu.VMEM)
    smem = pl.BlockSpec(memory_space=pltpu.SMEM)
    total = 2 * plane
    width = 256
    rows = each * local
    dma = pltpu.SemaphoreType.DMA
    out = pl.pallas_call(
        functools.partial(block_kernel, ("gz", "ea", ndev)),
        out_shape=jax.ShapeDtypeStruct((2, local, each * count), F32),
        in_specs=[smem, smem, smem, vmem, vmem, pl.BlockSpec(memory_space=pl.ANY)],
        out_specs=vmem,
        scratch_shapes=[
            pltpu.VMEM(peram.shape, F32),
            pltpu.VMEM((3, 2, count, count), F32),
            pltpu.VMEM((4, 2 * local, 6 * plane), BF16),
            pltpu.VMEM((2,) + links.shape, F32),
            pltpu.VMEM(links.shape[1:], F32),
            pltpu.VMEM((4, 6, local, plane), F32),
            pltpu.VMEM((9, local, total), F32),
            pltpu.VMEM((9, half, each, total), F32),
            pltpu.VMEM((6, 2 * count, total), BF16),
            pltpu.VMEM((rows, 2 * count), F32),
            pltpu.VMEM((6, rows, width), BF16),
            pltpu.VMEM((6, rows, width), BF16),
            pltpu.VMEM((half - 1, 2, local, each * count), BF16),
            pltpu.VMEM((half - 1, 2, local, each * count), BF16),
            dma((local // 16,)),
            dma((local // 16,)),
            dma((4,)),
            dma((4,)),
            dma,
            dma((2,)),
            dma,
            dma,
            dma((half - 1,)),
            dma((half - 1,)),
            dma((local // 16,)),
            dma((local // 16,)),
            dma((local // 16,)),
            dma((local // 16,)),
            dma,
        ],
        compiler_params=pltpu.CompilerParams(
            vmem_limit_bytes=62 * 1024 * 1024, collective_id=0, has_side_effects=True
        ),
        name="block",
    )(weights, momentum, spins.T, own, links, peram)
    return out


def solution(mesh):
    ndev = mesh.shape["gz"]
    in_specs = (
        P("ea", None, None, ("groups", "gz"), None),
        P(None, None, None, None, ("groups", "gz"), None),
        P("groups"),
        P("groups"),
        P("groups", None),
        P("groups", None, None, None, None),
    )
    out_specs = P("groups", "ea", "gz")

    def body(eigvec, links, momentum, weights, spins, peram):
        whole_rows = peram.shape[-1] % (2 * ndev) == 0 and ndev % 2 == 0 and ndev > 2
        whole_rows = whole_rows and eigvec.shape[0] % 16 == 0 and eigvec.shape[3] == 1
        run = shards if whole_rows else plain_shards
        return run(eigvec, links, momentum, weights, spins, peram)

    return jax.shard_map(body, mesh=mesh, in_specs=in_specs, out_specs=out_specs, check_vma=False)
```
